32 devices in a mesh: rep: 1 (over z), dp: 32 (over x, y, core).
Axes of the slice: x: 4, y: 4, z: 1, core: 2. Of those that a mesh axis runs over, the one named last changes fastest.
The devices are a block of a 4x4x8 slice.
Arguments:
- g_w_gate: bfloat16 [32, 2, 1024, 3200], P(('rep', 'dp'))
- g_w_up: bfloat16 [32, 2, 1024, 3200], P(('rep', 'dp'))
- g_w_down: bfloat16 [32, 2, 3200, 1024], P(('rep', 'dp'))
- w_gate: bfloat16 [2, 1024, 3200], replicated
- w_up: bfloat16 [2, 1024, 3200], replicated
- w_down: bfloat16 [2, 3200, 1024], replicated
- m_w_gate: float32 [2, 1024, 3200], P(None, 'dp')
- m_w_up: float32 [2, 1024, 3200], P(None, 'dp')
- m_w_down: float32 [2, 3200, 1024], P(None, 'dp')
- v_w_gate: float32 [2, 1024, 3200], P(None, 'dp')
- v_w_up: float32 [2, 1024, 3200], P(None, 'dp')
- v_w_down: float32 [2, 3200, 1024], P(None, 'dp')
Outputs:
- output 1: bfloat16 [2, 1024, 3200], P('rep')
- output 2: bfloat16 [2, 1024, 3200], P('rep')
- output 3: bfloat16 [2, 3200, 1024], P('rep')
- output 4: float32 [2, 1024, 3200], P('rep', 'dp')
- output 5: float32 [2, 1024, 3200], P('rep', 'dp')
- output 6: float32 [2, 3200, 1024], P('rep', 'dp')
- output 7: float32 [2, 1024, 3200], P('rep', 'dp')
- output 8: float32 [2, 1024, 3200], P('rep', 'dp')
- output 9: float32 [2, 3200, 1024], P('rep', 'dp')
All inputs are finite; a program needn't handle non-finite values.
Results may differ from the reference program's by a relative error of at most 0.022.
Values are sent between devices in bfloat16 or wider.
A program may use at most 768 MiB of HBM per device.

```python
import jax
import jax.numpy as jnp
from jax import lax

DEVICES = 32
D = 1024
FF = 3200
LAYERS = 2
NAMES = ("w_gate", "w_up", "w_down")
SHAPES = {"w_gate": (LAYERS, D, FF), "w_up": (LAYERS, D, FF), "w_down": (LAYERS, FF, D)}


def setup_inputs(seed: int = 0, part: int = 0) -> dict:
    kz, *keys = jax.random.split(jax.random.key(seed), 1 + 5 * len(NAMES))
    loud = 2.0 ** jax.random.uniform(kz, (), jnp.float32, -1.0, 1.0)
    drawn = {}
    for name, key, both in zip(NAMES, keys[:3], keys[3:6], strict=True):
        own = jax.random.normal(jax.random.fold_in(key, part), (DEVICES, *SHAPES[name]), jnp.float32)
        shared = jax.random.normal(jax.random.fold_in(both, part), SHAPES[name], jnp.float32)
        drawn["g_" + name] = (loud * (0.7 * shared / DEVICES + 0.7 * own * DEVICES**-0.5)).astype(jnp.bfloat16)
    for name, key in zip(NAMES, keys[6:9], strict=True):
        drawn[name] = (jax.random.normal(key, SHAPES[name], jnp.float32) * SHAPES[name][1] ** -0.5).astype(jnp.bfloat16)
    for name, key in zip(NAMES, keys[9:12], strict=True):
        drawn["m_" + name] = loud * 0.5 * jax.random.normal(key, SHAPES[name], jnp.float32)
    for name, key in zip(NAMES, keys[12:15], strict=True):
        drawn["v_" + name] = loud * loud * jax.random.uniform(key, SHAPES[name], jnp.float32, 0.5, 1.5)
    return drawn


def adamw(w, m, v, g):
    m = 0.9 * m + 0.1 * g
    v = 0.95 * v + 0.05 * g * g
    step = m * lax.rsqrt(v + 1e-8) + 0.1 * w
    return (w - 0.02 * step).astype(jnp.bfloat16), m, v


def reference(g_w_gate, g_w_up, g_w_down, w_gate, w_up, w_down, m_w_gate, m_w_up, m_w_down, v_w_gate, v_w_up, v_w_down):
    def total(terms):
        return lax.scan(lambda so_far, term: (so_far + term.astype(jnp.float32), None), jnp.zeros(terms.shape[1:], jnp.float32), terms)[0]

    gradients = [total(terms).astype(jnp.bfloat16).astype(jnp.float32) for terms in (g_w_gate, g_w_up, g_w_down)]
    new = [
        adamw(w.astype(jnp.float32), m, v, g)
        for w, m, v, g in zip((w_gate, w_up, w_down), (m_w_gate, m_w_up, m_w_down), (v_w_gate, v_w_up, v_w_down), gradients, strict=True)
    ]
    return tuple(one[which] for which in range(3) for one in new)
```

```python
import functools
import math

import jax
import jax.numpy as jnp
from jax import lax
from jax.experimental import pallas as pl
from jax.experimental.pallas import tpu as pltpu
from jax.sharding import PartitionSpec as P

MESH = pl.DeviceIdType.MESH
F32, BF16 = jnp.float32, jnp.bfloat16
SLOTS = 16
AHEAD = 12


def adamw(w, m, v, g):
    m = 0.9 * m + 0.1 * g
    v = 0.95 * v + 0.05 * g * g
    step = m * lax.rsqrt(v + 1e-8) + 0.1 * w
    return w - 0.02 * step, m, v


def step_kernel(n, *refs):
    g, w, m, v = (refs[i : i + 3] for i in (0, 3, 6, 9))
    ow, om, ov = (refs[i : i + 3] for i in (12, 15, 18))
    own, wsl = refs[21:24], refs[24:27]
    xg, xw, yw, zw, tmp = refs[27:32]
    ring_send, ring_recv, core_send, core_recv, all_recv, own_sem, in_sem, x_sems, ready = refs[32:]

    side = math.isqrt(n // 2)
    last = side - 1
    chips = side * side
    rows = m[0].shape[1]
    half = rows // 2
    tall = 2 * m[2].shape[1]
    low = m[2].shape[1]
    off = low // 8 * 8
    frame = tall - off
    shift = low - off
    quarter = ow[2].shape[2] // 4
    unit = 3 * half
    total = 4 * chips

    me = lax.axis_index("dp")
    k = lax.rem(me, 2)
    chip = lax.div(me, 2)
    x, y = lax.div(chip, side), lax.rem(chip, side)
    partner = me + 1 - 2 * k

    def wrap(z):
        return lax.rem(z + 2 * side, side)

    class Colour:
        def __init__(self, q):
            self.q = q
            self.l = a = lax.div(q, 2)
            self.h = lax.rem(q, 2)
            self.dir = 1 - 2 * self.h
            self.p1, self.p2 = x + a * (y - x), y + a * (x - y)
            self.a = a

        def chip(self, u, v):
            u, v = wrap(u), wrap(v)
            return (u + self.a * (v - u)) * side + v + self.a * (u - v)

        def next1(self):
            return self.chip(self.p1 + self.dir, self.p2) * 2 + k

        def next2(self):
            return self.chip(self.p1, self.p2 + self.dir) * 2 + k

        def back(self, i, j):
            return self.chip(self.p1 - self.dir * i, self.p2 - self.dir * j)

    def place(p, at, core, col):
        if p < 2:
            return (col.l, pl.ds(pl.multiple_of(at * (2 * rows) + core * rows + col.h * half, half), half))
        return (
            col.l,
            pl.ds(pl.multiple_of(at * tall, 8), tall),
            pl.ds(pl.multiple_of(core * (2 * quarter) + col.h * quarter, quarter), quarter),
        )

    def remote(src, dst, send, recv, device):
        return pltpu.make_async_remote_copy(
            src_ref=src, dst_ref=dst, send_sem=send, recv_sem=recv, device_id={"dp": device}, device_id_type=MESH
        )

    def wait_bytes(sem, chunks):
        part = ow[0].at[0, pl.ds(0, chunks * unit)]
        pltpu.make_async_copy(part, part, sem).wait()

    def wait_piece(p, sem):
        part = ow[0].at[0, pl.ds(0, half)]
        pltpu.make_async_copy(part, part, sem).wait()

    def chunk(t):
        s, j, col = lax.div(t, 4 * side), lax.rem(lax.div(t, 4), side), Colour(lax.rem(t, 4))
        return col, col.back(1 + s, 1 + j)

    def to_partner(t):
        col, at = chunk(t)
        for p in range(3):
            i = place(p, at, 1 - k, col)
            remote(g[p].at[(0, *i)], ow[p].at[i], core_send.at[col.q], core_recv.at[t], partner).start()

    def load_own(t):
        col, at = chunk(t)
        slot = lax.rem(t, SLOTS)
        for p in range(3):
            pltpu.make_async_copy(g[p].at[(0, *place(p, at, k, col))], own[p].at[slot], own_sem.at[slot]).start()

    def wait_own(slot):
        part = own[0].at[pl.ds(0, 3)]
        pltpu.make_async_copy(part, part, own_sem.at[slot]).wait()

    def each(count, body):
        lax.fori_loop(0, count, lambda i, c: (body(i), c)[1], 0)

    peers = [
        (wrap(x + dx) * side + wrap(y + dy)) * 2 + k for dx, dy in ((1, 0), (-1, 0), (0, 1), (0, -1))
    ] + [partner]
    barrier = pltpu.get_barrier_semaphore()
    for peer in peers:
        pl.semaphore_signal(barrier, inc=1, device_id={"dp": peer}, device_id_type=MESH)
    each(SLOTS, load_own)
    pl.semaphore_wait(barrier, len(peers))
    each(AHEAD, to_partner)

    loads = []
    for p in range(3):
        if p < 2:
            part = w[p].at[:, pl.ds(pl.multiple_of(me * rows, rows), rows)]
        else:
            part = w[p].at[:, pl.ds(pl.multiple_of(chip * tall + off * k, 8), frame)]
        loads.append(pltpu.make_async_copy(part, wsl[p], in_sem.at[p]))
        loads.append(pltpu.make_async_copy(m[p], om[p], in_sem.at[3 + p]))
        loads.append(pltpu.make_async_copy(v[p], ov[p], in_sem.at[6 + p]))
    for copy in loads:
        copy.start()

    def reduce_chunk(t, s, j, col, second):
        at = col.back(1 + s, 1 + j)
        slot = lax.rem(t, SLOTS)
        wait_bytes(core_recv.at[t], 1)
        wait_own(slot)
        first = not isinstance(s, int) or s > 0
        for p in range(3):
            i = place(p, at, k, col)
            so_far = ow[p][i].astype(F32) + own[p][slot].astype(F32)
            if first:
                r = (s - 1) * side + j
                wait_piece(p, ring_recv.at[col.q, r, p])
                so_far += ow[p][place(p, r, 1 - k, col)].astype(F32)
            if second and j > 0:
                r = last * side + j - 1
                wait_piece(p, ring_recv.at[col.q, r, p])
                so_far += ow[p][place(p, r, 1 - k, col)].astype(F32)
            ow[p][i] = so_far.astype(BF16)
        if second and j == last:
            return
        for p in range(3):
            i = place(p, at, k, col)
            r = s * side + j
            there = ow[p].at[place(p, r, 1 - k, col)]
            device = col.next2() if second else col.next1()
            remote(ow[p].at[i], there, ring_send.at[col.q], ring_recv.at[col.q, r, p], device).start()

    def refill(t):
        @pl.when(t + SLOTS < total)
        def _():
            load_own(t + SLOTS)

        @pl.when(t + AHEAD < total)
        def _():
            to_partner(t + AHEAD)

    def round_zero(i):
        reduce_chunk(i, 0, lax.div(i, 4), Colour(lax.rem(i, 4)), False)
        refill(i)

    def round_more(i):
        t = i + 4 * side
        reduce_chunk(t, lax.div(t, 4 * side), lax.rem(lax.div(t, 4), side), Colour(lax.rem(t, 4)), False)
        refill(t)

    each(4 * side, round_zero)
    each(4 * side * (last - 1), round_more)
    for j in range(side):

        def round_last(q):
            t = (last * side + j) * 4 + q
            reduce_chunk(t, last, j, Colour(q), True)
            refill(t)

        each(4, round_last)

    def swap(q):
        col = Colour(q)
        part = ow[2].at[
            col.l,
            pl.ds(pl.multiple_of(chip * tall + off * (1 - k), 8), frame),
            pl.ds(pl.multiple_of(k * (2 * quarter) + col.h * quarter, quarter), quarter),
        ]
        return remote(part, xg.at[q], x_sems.at[0, q], x_sems.at[1, q], partner)

    each(4, lambda q: swap(q).start())

    for q in range(4):
        wait_bytes(ring_send.at[q], chips - 1)
        wait_bytes(core_send.at[q], chips)
    for peer in peers:
        pl.semaphore_signal(ready, inc=1, device_id={"dp": peer}, device_id_type=MESH)
    for copy in loads:
        copy.wait()

    def wide_step(q):
        col = Colour(q)
        here = pl.ds(pl.multiple_of(col.h * half, half), half)
        for p in range(2):
            i = place(p, chip, k, col)
            new, new_m, new_v = adamw(
                wsl[p][col.l, here].astype(F32), om[p][col.l, here], ov[p][col.l, here], ow[p][i].astype(F32)
            )
            ow[p][i] = new.astype(BF16)
            om[p][col.l, here] = new_m
            ov[p][col.l, here] = new_v

    def spread(q, i, j, pieces):
        col = Colour(q)
        at = col.back(i, j)
        for p in pieces:
            if i + j > 0:
                wait_piece(p, ring_recv.at[q, i * side + j, p])
            part = ow[p].at[place(p, at, k, col)]
            if i == 0 and j < last:
                remote(part, part, ring_send.at[q], ring_recv.at[q, j + 1, p], col.next2()).start()
            if i < last:
                remote(part, part, ring_send.at[q], ring_recv.at[q, (i + 1) * side + j, p], col.next1()).start()
            remote(part, part, core_send.at[q], all_recv.at[q], partner).start()

    each(4, wide_step)
    pl.semaphore_wait(ready, len(peers))
    each(4, lambda q: spread(q, 0, 0, (0, 1)))

    def give(q):
        return remote(zw.at[q], xw.at[q], x_sems.at[2, q], x_sems.at[3, q], partner)

    def tall_step(q):
        col = Colour(q)
        swap(q).wait()
        for core in range(2):

            @pl.when(k == core)
            def _():
                for mine in (True, False):
                    side_of = core if mine else 1 - core
                    cols = pl.ds(pl.multiple_of(side_of * 2 * quarter + col.h * quarter, quarter), quarter)
                    if mine:
                        grad = ow[2][col.l, pl.ds(pl.multiple_of(chip * tall + off * core, 8), frame), cols]
                    else:
                        grad = xg[q]
                    at = slice(shift * core, shift * core + low)
                    new, new_m, new_v = adamw(
                        wsl[2][col.l, :, cols].astype(F32)[at],
                        om[2][col.l, :, cols],
                        ov[2][col.l, :, cols],
                        grad.astype(F32)[at],
                    )
                    om[2][col.l, :, cols] = new_m
                    ov[2][col.l, :, cols] = new_v
                    tmp[at, :] = new
                    (yw if mine else zw)[q] = tmp[...]

        give(q).start()

    tmp[...] = jnp.zeros_like(tmp)
    each(4, tall_step)

    def join(q):
        col = Colour(q)
        give(q).wait()
        cols = pl.ds(pl.multiple_of(k * 2 * quarter + col.h * quarter, quarter), quarter)
        base = chip * tall

        def put(start, value):
            ow[2][col.l, pl.ds(pl.multiple_of(base + start, 8), value.shape[0]), cols] = value.astype(BF16)

        for core in range(2):

            @pl.when(k == core)
            def _():
                top, bottom = (yw, xw) if core == 0 else (xw, yw)
                put(0, top[q, 0:off, :])
                row = lax.broadcasted_iota(jnp.int32, (8, quarter), 0)
                put(off, jnp.where(row < shift, top[q, off : off + 8, :], bottom[q, 0:8, :]))
                put(off + 8, bottom[q, 8:frame, :])

        spread(q, 0, 0, (2,))

    each(4, join)

    order = [(0, 1), (1, 0), (0, 2), (1, 1), (0, 3), (1, 2), (1, 3)]
    order += [(i, j) for i in range(2, side) for j in range(side)]
    order = [(i, j) for i, j in order if i < side and j < side]
    for i, j in order:
        each(4, lambda q, i=i, j=j: spread(q, i, j, (0, 1, 2)))
    for q in range(4):
        wait_bytes(ring_send.at[q], chips - 1)
        wait_bytes(core_send.at[q], chips)
        wait_bytes(all_recv.at[q], chips)


def drain_kernel(count, *refs):
    sem = refs[-1]
    copies = [pltpu.make_async_copy(refs[i], refs[count + i], sem.at[i]) for i in range(count)]
    for copy in copies:
        copy.start()
    for copy in copies:
        copy.wait()


def drain(arrays):
    count = len(arrays)
    return list(
        pl.pallas_call(
            functools.partial(drain_kernel, count),
            out_shape=[jax.ShapeDtypeStruct(a.shape, a.dtype) for a in arrays],
            in_specs=[pl.BlockSpec(memory_space=pltpu.VMEM)] * count,
            out_specs=[pl.BlockSpec(memory_space=pl.ANY)] * count,
            scratch_shapes=[pltpu.SemaphoreType.DMA((count,))],
            compiler_params=pltpu.CompilerParams(vmem_limit_bytes=1 << 20),
        )(*arrays)
    )


def solution(mesh):
    n = mesh.shape["dp"]

    def step(*arrays):
        g, w, m, v = (arrays[i : i + 3] for i in (0, 3, 6, 9))
        rows, wide = m[0].shape[1:]
        low, narrow = m[2].shape[1:]
        side = math.isqrt(n // 2)
        half, quarter = rows // 2, narrow // 4
        frame = 2 * low - low // 8 * 8
        assert half * wide == 2 * low * quarter and side * side * 2 == n and low % 8
        dma, regular = pltpu.SemaphoreType.DMA, pltpu.SemaphoreType.REGULAR
        outs = pl.pallas_call(
            functools.partial(step_kernel, n),
            out_shape=[pltpu.VMEM(a.shape, a.dtype) for a in (*w, *m, *v)],
            in_specs=[pl.BlockSpec(memory_space=pltpu.HBM)] * 12,
            out_specs=[pl.BlockSpec(memory_space=pltpu.VMEM)] * 9,
            scratch_shapes=[
                pltpu.VMEM((SLOTS, half, wide), BF16),
                pltpu.VMEM((SLOTS, half, wide), BF16),
                pltpu.VMEM((SLOTS, 2 * low, quarter), BF16),
                pltpu.VMEM((2, rows, wide), BF16),
                pltpu.VMEM((2, rows, wide), BF16),
                pltpu.VMEM((2, frame, narrow), BF16),
                pltpu.VMEM((4, frame, quarter), BF16),
                pltpu.VMEM((4, frame, quarter), F32),
                pltpu.VMEM((4, frame, quarter), F32),
                pltpu.VMEM((4, frame, quarter), F32),
                pltpu.VMEM((frame, quarter), F32),
                dma((4,)),
                dma((4, side * side, 3)),
                dma((4,)),
                dma((4 * side * side,)),
                dma((4,)),
                dma((SLOTS,)),
                dma((9,)),
                dma((4, 4)),
                regular,
            ],
            compiler_params=pltpu.CompilerParams(
                collective_id=0, has_side_effects=True, vmem_limit_bytes=14 << 20
            ),
        )(*g, *w, *m, *v)
        outs = [*drain(outs[0:1]), *drain(outs[1:2]), *drain(outs[2:3]), *drain(outs[3:])]
        return tuple(outs)

    all_of, cut = P(None, None, None), P(None, "dp", None)
    return jax.shard_map(
        step,
        mesh=mesh,
        in_specs=(P(("rep", "dp"), None, None, None),) * 3 + (all_of,) * 3 + (cut,) * 6,
        out_specs=(P("rep", None, None),) * 3 + (P("rep", "dp", None),) * 6,
        check_vma=False,
    )
```

```python
import functools
import math

import jax
import jax.numpy as jnp
from jax import lax
from jax.experimental import pallas as pl
from jax.experimental.pallas import tpu as pltpu
from jax.sharding import PartitionSpec as P

MESH = pl.DeviceIdType.MESH
F32, BF16 = jnp.float32, jnp.bfloat16
SLOTS = 16
PARTS = 8
STAGES = (2, 0, 1)


def adamw(w, m, v, g):
    m = 0.9 * m + 0.1 * g
    v = 0.95 * v + 0.05 * g * g
    step = m * lax.rsqrt(v + 1e-8) + 0.1 * w
    return w - 0.02 * step, m, v


def step_kernel(n, *refs):
    g, w, m, v = (refs[i : i + 3] for i in (0, 3, 6, 9))
    ow, om, ov = (refs[i : i + 3] for i in (12, 15, 18))
    own, wsl = refs[21:24], refs[24:27]
    xg, xw, yw, zw, tmp = refs[27:32]
    ring_send, ring_recv, core_send, core_recv, all_recv, own_sem, in_sem, x_sems, ready = refs[32:]

    side = math.isqrt(n // 2)
    last = side - 1
    chips = side * side
    rows = m[0].shape[1]
    half = rows // 2
    low = m[2].shape[0]
    tall = 2 * low
    off = low // 8 * 8
    frame = tall - off
    shift = low - off
    quarter = ow[2].shape[2] // 4
    total = 4 * chips
    ahead = 4 * side

    me = lax.axis_index("dp")
    k = lax.rem(me, 2)
    chip = lax.div(me, 2)
    x, y = lax.div(chip, side), lax.rem(chip, side)
    partner = me + 1 - 2 * k

    def wrap(z):
        return lax.rem(z + 2 * side, side)

    class Colour:
        def __init__(self, q):
            self.q = q
            self.l = a = lax.div(q, 2)
            self.h = lax.rem(q, 2)
            self.dir = 1 - 2 * self.h
            self.p1, self.p2 = x + a * (y - x), y + a * (x - y)
            self.a = a

        def chip(self, u, v):
            u, v = wrap(u), wrap(v)
            return (u + self.a * (v - u)) * side + v + self.a * (u - v)

        def next1(self):
            return self.chip(self.p1 + self.dir, self.p2) * 2 + k

        def next2(self):
            return self.chip(self.p1, self.p2 + self.dir) * 2 + k

        def back(self, i, j):
            return self.chip(self.p1 - self.dir * i, self.p2 - self.dir * j)

    def place(p, at, core, col):
        if p < 2:
            return (col.l, pl.ds(pl.multiple_of(at * (2 * rows) + core * rows + col.h * half, half), half))
        return (
            col.l,
            pl.ds(pl.multiple_of(at * tall, 8), tall),
            pl.ds(pl.multiple_of(core * (2 * quarter) + col.h * quarter, quarter), quarter),
        )

    def remote(src, dst, send, recv, device):
        return pltpu.make_async_remote_copy(
            src_ref=src, dst_ref=dst, send_sem=send, recv_sem=recv, device_id={"dp": device}, device_id_type=MESH
        )

    def wait_pieces(sem, count):
        part = ow[0].at[0, pl.ds(0, count * half)]
        pltpu.make_async_copy(part, part, sem).wait()

    def split(t):
        s, j, col = lax.div(t, 4 * side), lax.rem(lax.div(t, 4), side), Colour(lax.rem(t, 4))
        return col, col.back(1 + s, 1 + j)

    def to_partner(p, t):
        col, at = split(t)
        i = place(p, at, 1 - k, col)
        remote(g[p].at[(0, *i)], ow[p].at[i], core_send.at[p, col.q], core_recv.at[p, t], partner).start()

    def load_own(p, t):
        col, at = split(t)
        slot = lax.rem(t, SLOTS)
        pltpu.make_async_copy(g[p].at[(0, *place(p, at, k, col))], own[p].at[slot], own_sem.at[p, slot]).start()

    def each(count, body):
        lax.fori_loop(0, count, lambda i, c: (body(i), c)[1], 0)

    peers = [
        (wrap(x + dx) * side + wrap(y + dy)) * 2 + k for dx, dy in ((1, 0), (-1, 0), (0, 1), (0, -1))
    ] + [partner]
    barrier = pltpu.get_barrier_semaphore()
    for peer in peers:
        pl.semaphore_signal(barrier, inc=1, device_id={"dp": peer}, device_id_type=MESH)
    for p in STAGES:
        each(SLOTS, functools.partial(load_own, p))
    pl.semaphore_wait(barrier, len(peers))
    each(ahead, functools.partial(to_partner, STAGES[0]))

    loads = []
    for p in range(3):
        if p < 2:
            part = w[p].at[:, pl.ds(pl.multiple_of(me * rows, rows), rows)]
        else:
            part = w[p].at[:, pl.ds(pl.multiple_of(chip * tall + off * k, 8), frame)]
        loads.append(pltpu.make_async_copy(part, wsl[p], in_sem.at[p]))
        loads.append(pltpu.make_async_copy(m[p], om[p], in_sem.at[3 + p]))
        loads.append(pltpu.make_async_copy(v[p], ov[p], in_sem.at[6 + p]))
    for copy in loads:
        copy.start()

    def reduce(p, s, j, q):
        col = Colour(q)
        at = col.back(1 + s, 1 + j)
        t = (s * side + j) * 4 + q
        slot = lax.rem(t, SLOTS)
        second = isinstance(s, int) and s == last
        i = place(p, at, k, col)
        wait_pieces(core_recv.at[p, t], 1)
        wait_pieces(own_sem.at[p, slot], 1)
        so_far = ow[p][i].astype(F32) + own[p][slot].astype(F32)
        came = []
        if not isinstance(s, int) or s > 0:
            came.append((s - 1) * side + j)
        if second and j > 0:
            came.append(last * side + j - 1)
        for r in came:
            wait_pieces(ring_recv.at[p, q, r], 1)
            so_far += ow[p][place(p, r, 1 - k, col)].astype(F32)
        ow[p][i] = so_far.astype(BF16)
        if not (second and j == last):
            r = s * side + j
            there = ow[p].at[place(p, r, 1 - k, col)]
            device = col.next2() if second else col.next1()
            remote(ow[p].at[i], there, ring_send.at[p, q], ring_recv.at[p, q, r], device).start()

        @pl.when(t + SLOTS < total)
        def _():
            load_own(p, t + SLOTS)

        @pl.when(t + ahead < total)
        def _():
            to_partner(p, t + ahead)

        if p != STAGES[-1]:

            @pl.when((t >= total - 2 * ahead) & (t < total - ahead))
            def _():
                to_partner(STAGES[STAGES.index(p) + 1], t + 2 * ahead - total)

    def round_of(p, s):
        each(4 * side, lambda i: reduce(p, s, lax.div(i, 4), lax.rem(i, 4)))

    def few(p, s, j):
        each(4, lambda q: reduce(p, s, j, q))

    def let_in(p):
        for q in range(4):
            wait_pieces(ring_send.at[p, q], chips - 1)
            wait_pieces(core_send.at[p, q], chips)
        for peer in peers:
            pl.semaphore_signal(ready.at[p], inc=1, device_id={"dp": peer}, device_id_type=MESH)

    def spread(p, i, j, q):
        col = Colour(q)
        at = col.back(i, j)
        if i + j > 0:
            wait_pieces(ring_recv.at[p, q, i * side + j], 1)
        part = ow[p].at[place(p, at, k, col)]
        if i == 0 and j < last:
            remote(part, part, ring_send.at[p, q], ring_recv.at[p, q, j + 1], col.next2()).start()
        if i < last:
            remote(part, part, ring_send.at[p, q], ring_recv.at[p, q, (i + 1) * side + j], col.next1()).start()
        remote(part, part, core_send.at[p, q], all_recv.at[p, q], partner).start()

    def wide_step(p, q):
        col = Colour(q)
        here = pl.ds(pl.multiple_of(col.h * half, half), half)
        i = place(p, chip, k, col)
        new, new_m, new_v = adamw(
            wsl[p][col.l, here].astype(F32), om[p][col.l, here], ov[p][col.l, here], ow[p][i].astype(F32)
        )
        ow[p][i] = new.astype(BF16)
        om[p][col.l, here] = new_m
        ov[p][col.l, here] = new_v

    def swap(q):
        col = Colour(q)
        part = ow[2].at[
            col.l,
            pl.ds(pl.multiple_of(chip * tall + off * (1 - k), 8), frame),
            pl.ds(pl.multiple_of(k * (2 * quarter) + col.h * quarter, quarter), quarter),
        ]
        return remote(part, xg.at[q], x_sems.at[0, q], x_sems.at[1, q], partner)

    def give(q):
        return remote(zw.at[q], xw.at[q], x_sems.at[2, q], x_sems.at[3, q], partner)

    def tall_step(q):
        l, h = q // 2, q % 2
        swap(q).wait()
        for core in range(2):

            @pl.when(k == core)
            def _():
                for mine in (True, False):
                    side_of = core if mine else 1 - core
                    cols = pl.ds(side_of * 2 * quarter + h * quarter, quarter)
                    if mine:
                        grad = ow[2][l, pl.ds(pl.multiple_of(chip * tall + off * core, 8), frame), cols]
                    else:
                        grad = xg[q]
                    at = slice(shift * core, shift * core + low)
                    new, new_m, new_v = adamw(
                        wsl[2][l, :, cols].astype(F32)[at],
                        om[2][:, l, cols],
                        ov[2][:, l, cols],
                        grad.astype(F32)[at],
                    )
                    om[2][:, l, cols] = new_m
                    ov[2][:, l, cols] = new_v
                    tmp[at, :] = new
                    (yw if mine else zw)[q] = tmp[...]

        give(q).start()

    def join(q):
        col = Colour(q)
        give(q).wait()
        cols = pl.ds(pl.multiple_of(k * 2 * quarter + col.h * quarter, quarter), quarter)
        base = chip * tall

        def put(start, value):
            ow[2][col.l, pl.ds(pl.multiple_of(base + start, 8), value.shape[0]), cols] = value.astype(BF16)

        for core in range(2):

            @pl.when(k == core)
            def _():
                top, bottom = (yw, xw) if core == 0 else (xw, yw)
                put(0, top[q, 0:off, :])
                row = lax.broadcasted_iota(jnp.int32, (8, quarter), 0)
                put(off, jnp.where(row < shift, top[q, off : off + 8, :], bottom[q, 0:8, :]))
                put(off + 8, bottom[q, 8:frame, :])

    first, middle, final = STAGES
    assert first == 2
    tmp[...] = jnp.zeros_like(tmp)

    round_of(first, 0)
    each(last - 1, lambda s: round_of(first, s + 1))
    for j in range(side):
        few(middle, 0, j)
        few(first, last, j)
    each(4, lambda q: swap(q).start())
    round_of(middle, 1)
    let_in(first)
    for copy in loads:
        copy.wait()
    for q in range(4):
        tall_step(q)
    each(last - 2, lambda s: round_of(middle, s + 2))
    each(4, join)
    for j in range(side):
        few(final, 0, j)
        few(middle, last, j)
    round_of(final, 1)
    let_in(middle)
    each(4, lambda q: wide_step(middle, q))
    each(last - 2, lambda s: round_of(final, s + 2))
    few(final, last, 0)
    pl.semaphore_wait(ready.at[first], len(peers))
    each(4, lambda q: spread(first, 0, 0, q))
    few(final, last, 1)
    pl.semaphore_wait(ready.at[middle], len(peers))
    each(4, lambda q: spread(middle, 0, 0, q))
    for j in range(2, side):
        few(final, last, j)
    let_in(final)
    each(4, lambda q: spread(first, 0, 1, q))
    each(4, lambda q: wide_step(final, q))
    pl.semaphore_wait(ready.at[final], len(peers))
    each(4, lambda q: spread(final, 0, 0, q))

    order = [(0, 1), (1, 0), (0, 2), (1, 1), (0, 3), (1, 2), (1, 3)]
    order += [(i, j) for i in range(2, side) for j in range(side)]
    order = [(i, j) for i, j in order if i < side and j < side]
    for i, j in order:
        for p in STAGES:
            if (p, i, j) != (first, 0, 1):
                each(4, lambda q, p=p, i=i, j=j: spread(p, i, j, q))
    for p in range(3):
        for q in range(4):
            wait_pieces(ring_send.at[p, q], chips - 1)
            wait_pieces(core_send.at[p, q], chips)
            wait_pieces(all_recv.at[p, q], chips)


def drain_kernel(count, *refs):
    sem = refs[-1]
    copies = []
    for i in range(count):
        here, there = refs[i], refs[count + i]
        parts = PARTS if here.shape[1] % (8 * PARTS) == 0 else 1
        size = here.shape[1] // parts
        for a in range(here.shape[0] if parts > 1 else 1):
            for b in range(parts):
                at = (a, pl.ds(b * size, size)) if parts > 1 else (slice(None),)
                copies.append(pltpu.make_async_copy(here.at[at], there.at[at], sem.at[len(copies)]))
    for copy in copies:
        copy.start()
    for copy in copies:
        copy.wait()


def drain(arrays):
    count = len(arrays)
    return list(
        pl.pallas_call(
            functools.partial(drain_kernel, count),
            out_shape=[jax.ShapeDtypeStruct(a.shape, a.dtype) for a in arrays],
            in_specs=[pl.BlockSpec(memory_space=pltpu.VMEM)] * count,
            out_specs=[pl.BlockSpec(memory_space=pl.ANY)] * count,
            scratch_shapes=[pltpu.SemaphoreType.DMA((2 * PARTS * count,))],
            compiler_params=pltpu.CompilerParams(vmem_limit_bytes=1 << 20),
        )(*arrays)
    )


def solution(mesh):
    n = mesh.shape["dp"]

    def step(*arrays):
        g, w, m, v = (list(arrays[i : i + 3]) for i in (0, 3, 6, 9))
        m[2], v[2] = m[2].swapaxes(0, 1), v[2].swapaxes(0, 1)
        rows, wide = m[0].shape[1:]
        low, _, narrow = m[2].shape
        side = math.isqrt(n // 2)
        half, quarter = rows // 2, narrow // 4
        frame = 2 * low - low // 8 * 8
        assert half * wide == 2 * low * quarter and side * side * 2 == n and low % 8
        dma, regular = pltpu.SemaphoreType.DMA, pltpu.SemaphoreType.REGULAR
        outs = pl.pallas_call(
            functools.partial(step_kernel, n),
            out_shape=[pltpu.VMEM(a.shape, a.dtype) for a in (*w, *m, *v)],
            in_specs=[pl.BlockSpec(memory_space=pltpu.HBM)] * 12,
            out_specs=[pl.BlockSpec(memory_space=pltpu.VMEM)] * 9,
            scratch_shapes=[
                pltpu.VMEM((SLOTS, half, wide), BF16),
                pltpu.VMEM((SLOTS, half, wide), BF16),
                pltpu.VMEM((SLOTS, 2 * low, quarter), BF16),
                pltpu.VMEM((2, rows, wide), BF16),
                pltpu.VMEM((2, rows, wide), BF16),
                pltpu.VMEM((2, frame, narrow), BF16),
                pltpu.VMEM((4, frame, quarter), BF16),
                pltpu.VMEM((4, frame, quarter), F32),
                pltpu.VMEM((4, frame, quarter), F32),
                pltpu.VMEM((4, frame, quarter), F32),
                pltpu.VMEM((frame, quarter), F32),
                dma((3, 4)),
                dma((3, 4, side * side)),
                dma((3, 4)),
                dma((3, 4 * side * side)),
                dma((3, 4)),
                dma((3, SLOTS)),
                dma((9,)),
                dma((4, 4)),
                regular((3,)),
            ],
            compiler_params=pltpu.CompilerParams(
                collective_id=0, has_side_effects=True, vmem_limit_bytes=14 << 20
            ),
        )(*g, *w, *m, *v)
        outs = [*drain(outs[0:1]), *drain(outs[1:2]), *drain(outs[2:3]), *drain(outs[3:])]
        for i in (5, 8):
            outs[i] = outs[i].swapaxes(0, 1)
        return tuple(outs)

    all_of, cut = P(None, None, None), P(None, "dp", None)
    return jax.shard_map(
        step,
        mesh=mesh,
        in_specs=(P(("rep", "dp"), None, None, None),) * 3 + (all_of,) * 3 + (cut,) * 6,
        out_specs=(P("rep", None, None),) * 3 + (P("rep", "dp", None),) * 6,
        check_vma=False,
    )
```

```python
import functools
import math

import jax
import jax.numpy as jnp
from jax import lax
from jax.experimental import pallas as pl
from jax.experimental.pallas import tpu as pltpu
from jax.sharding import PartitionSpec as P

MESH = pl.DeviceIdType.MESH
F32, BF16 = jnp.float32, jnp.bfloat16
SLOTS = 16
PARTS = 8
STAGES = (2, 0, 1)


def adamw(w, m, v, g):
    m = 0.9 * m + 0.1 * g
    v = 0.95 * v + 0.05 * g * g
    step = m * lax.rsqrt(v + 1e-8) + 0.1 * w
    return w - 0.02 * step, m, v


def step_kernel(n, *refs):
    g, w, m, v = (refs[i : i + 3] for i in (0, 3, 6, 9))
    ow, om, ov = (refs[i : i + 3] for i in (12, 15, 18))
    own, wsl = refs[21:24], refs[24:27]
    xg, xw, yw, zw, tmp = refs[27:32]
    ring_send, ring_recv, core_send, core_recv, all_recv, own_sem, in_sem, x_sems, ready = refs[32:]

    side = math.isqrt(n // 2)
    last = side - 1
    chips = side * side
    rows = m[0].shape[1]
    half = rows // 2
    low = m[2].shape[0]
    tall = 2 * low
    off = low // 8 * 8
    frame = tall - off
    shift = low - off
    quarter = ow[2].shape[2] // 4
    total = 4 * chips
    ahead = 4 * side

    me = lax.axis_index("dp")
    k = lax.rem(me, 2)
    chip = lax.div(me, 2)
    x, y = lax.div(chip, side), lax.rem(chip, side)
    partner = me + 1 - 2 * k

    def wrap(z):
        return lax.rem(z + 2 * side, side)

    class Colour:
        def __init__(self, q):
            self.q = q
            self.l = a = lax.div(q, 2)
            self.h = lax.rem(q, 2)
            self.dir = 1 - 2 * self.h
            self.p1, self.p2 = x + a * (y - x), y + a * (x - y)
            self.a = a

        def chip(self, u, v):
            u, v = wrap(u), wrap(v)
            return (u + self.a * (v - u)) * side + v + self.a * (u - v)

        def next1(self):
            return self.chip(self.p1 + self.dir, self.p2) * 2 + k

        def next2(self):
            return self.chip(self.p1, self.p2 + self.dir) * 2 + k

        def back(self, i, j):
            return self.chip(self.p1 - self.dir * i, self.p2 - self.dir * j)

    def place(p, at, core, col):
        if p < 2:
            return (col.l, pl.ds(pl.multiple_of(at * (2 * rows) + core * rows + col.h * half, half), half))
        return (
            col.l,
            pl.ds(pl.multiple_of(at * tall, 8), tall),
            pl.ds(pl.multiple_of(core * (2 * quarter) + col.h * quarter, quarter), quarter),
        )

    def remote(src, dst, send, recv, device):
        return pltpu.make_async_remote_copy(
            src_ref=src, dst_ref=dst, send_sem=send, recv_sem=recv, device_id={"dp": device}, device_id_type=MESH
        )

    def wait_pieces(sem, count):
        part = ow[0].at[0, pl.ds(0, count * half)]
        pltpu.make_async_copy(part, part, sem).wait()

    def split(t):
        s, j, col = lax.div(t, 4 * side), lax.rem(lax.div(t, 4), side), Colour(lax.rem(t, 4))
        return col, col.back(1 + s, 1 + j)

    def to_partner(p, t):
        col, at = split(t)
        i = place(p, at, 1 - k, col)
        remote(g[p].at[(0, *i)], ow[p].at[i], core_send.at[p, col.q], core_recv.at[p, t], partner).start()

    def load_own(p, t):
        col, at = split(t)
        slot = lax.rem(t, SLOTS)
        pltpu.make_async_copy(g[p].at[(0, *place(p, at, k, col))], own[p].at[slot], own_sem.at[p, slot]).start()

    def each(count, body):
        lax.fori_loop(0, count, lambda i, c: (body(i), c)[1], 0)

    peers = [
        (wrap(x + dx) * side + wrap(y + dy)) * 2 + k for dx, dy in ((1, 0), (-1, 0), (0, 1), (0, -1))
    ] + [partner]
    barrier = pltpu.get_barrier_semaphore()
    for peer in peers:
        pl.semaphore_signal(barrier, inc=1, device_id={"dp": peer}, device_id_type=MESH)
    for p in STAGES:
        each(SLOTS, functools.partial(load_own, p))
    pl.semaphore_wait(barrier, len(peers))
    each(ahead, functools.partial(to_partner, STAGES[0]))

    loads = []
    for p in range(3):
        if p < 2:
            part = w[p].at[:, pl.ds(pl.multiple_of(me * rows, rows), rows)]
        else:
            part = w[p].at[:, pl.ds(pl.multiple_of(chip * tall + off * k, 8), frame)]
        loads.append(pltpu.make_async_copy(part, wsl[p], in_sem.at[p]))
        loads.append(pltpu.make_async_copy(m[p], om[p], in_sem.at[3 + p]))
        loads.append(pltpu.make_async_copy(v[p], ov[p], in_sem.at[6 + p]))
    for copy in loads:
        copy.start()

    def reduce(p, s, j, q):
        col = Colour(q)
        at = col.back(1 + s, 1 + j)
        t = (s * side + j) * 4 + q
        slot = lax.rem(t, SLOTS)
        second = isinstance(s, int) and s == last
        i = place(p, at, k, col)
        wait_pieces(core_recv.at[p, t], 1)
        wait_pieces(own_sem.at[p, slot], 1)
        so_far = ow[p][i].astype(F32) + own[p][slot].astype(F32)
        came = []
        if not isinstance(s, int) or s > 0:
            came.append((s - 1) * side + j)
        if second and j > 0:
            came.append(last * side + j - 1)
        for r in came:
            wait_pieces(ring_recv.at[p, q, r], 1)
            so_far += ow[p][place(p, r, 1 - k, col)].astype(F32)
        ow[p][i] = so_far.astype(BF16)
        if not (second and j == last):
            r = s * side + j
            there = ow[p].at[place(p, r, 1 - k, col)]
            device = col.next2() if second else col.next1()
            remote(ow[p].at[i], there, ring_send.at[p, q], ring_recv.at[p, q, r], device).start()

        @pl.when(t + SLOTS < total)
        def _():
            load_own(p, t + SLOTS)

        @pl.when(t + ahead < total)
        def _():
            to_partner(p, t + ahead)

        if p != STAGES[-1]:

            @pl.when((t >= total - 2 * ahead) & (t < total - ahead))
            def _():
                to_partner(STAGES[STAGES.index(p) + 1], t + 2 * ahead - total)

    def few(p, s, j):
        each(4, lambda q: reduce(p, s, j, q))

    def let_in(p):
        for q in range(4):
            wait_pieces(ring_send.at[p, q], chips - 1)
            wait_pieces(core_send.at[p, q], chips)
        for peer in peers:
            pl.semaphore_signal(ready.at[p], inc=1, device_id={"dp": peer}, device_id_type=MESH)

    def spread(p, i, j, q):
        col = Colour(q)
        at = col.back(i, j)
        if i + j > 0:
            wait_pieces(ring_recv.at[p, q, i * side + j], 1)
        part = ow[p].at[place(p, at, k, col)]
        if i == 0 and j < last:
            remote(part, part, ring_send.at[p, q], ring_recv.at[p, q, j + 1], col.next2()).start()
        if i < last:
            remote(part, part, ring_send.at[p, q], ring_recv.at[p, q, (i + 1) * side + j], col.next1()).start()
        remote(part, part, core_send.at[p, q], all_recv.at[p, q], partner).start()

    def wide_step(p, q):
        col = Colour(q)
        here = pl.ds(pl.multiple_of(col.h * half, half), half)
        i = place(p, chip, k, col)
        new, new_m, new_v = adamw(
            wsl[p][col.l, here].astype(F32), om[p][col.l, here], ov[p][col.l, here], ow[p][i].astype(F32)
        )
        ow[p][i] = new.astype(BF16)
        om[p][col.l, here] = new_m
        ov[p][col.l, here] = new_v

    def swap(q):
        col = Colour(q)
        part = ow[2].at[
            col.l,
            pl.ds(pl.multiple_of(chip * tall + off * (1 - k), 8), frame),
            pl.ds(pl.multiple_of(k * (2 * quarter) + col.h * quarter, quarter), quarter),
        ]
        return remote(part, xg.at[q], x_sems.at[0, q], x_sems.at[1, q], partner)

    def give(q):
        return remote(zw.at[q], xw.at[q], x_sems.at[2, q], x_sems.at[3, q], partner)

    def tall_step(q):
        l, h = q // 2, q % 2
        swap(q).wait()
        for core in range(2):

            @pl.when(k == core)
            def _():
                for mine in (True, False):
                    side_of = core if mine else 1 - core
                    cols = pl.ds(side_of * 2 * quarter + h * quarter, quarter)
                    if mine:
                        grad = ow[2][l, pl.ds(pl.multiple_of(chip * tall + off * core, 8), frame), cols]
                    else:
                        grad = xg[q]
                    at = slice(shift * core, shift * core + low)
                    new, new_m, new_v = adamw(
                        wsl[2][l, :, cols].astype(F32)[at],
                        om[2][:, l, cols],
                        ov[2][:, l, cols],
                        grad.astype(F32)[at],
                    )
                    om[2][:, l, cols] = new_m
                    ov[2][:, l, cols] = new_v
                    tmp[at, :] = new
                    (yw if mine else zw)[q] = tmp[...]

        give(q).start()

    def join(q):
        col = Colour(q)
        give(q).wait()
        cols = pl.ds(pl.multiple_of(k * 2 * quarter + col.h * quarter, quarter), quarter)
        base = chip * tall

        def put(start, value):
            ow[2][col.l, pl.ds(pl.multiple_of(base + start, 8), value.shape[0]), cols] = value.astype(BF16)

        for core in range(2):

            @pl.when(k == core)
            def _():
                top, bottom = (yw, xw) if core == 0 else (xw, yw)
                put(0, top[q, 0:off, :])
                row = lax.broadcasted_iota(jnp.int32, (8, quarter), 0)
                put(off, jnp.where(row < shift, top[q, off : off + 8, :], bottom[q, 0:8, :]))
                put(off + 8, bottom[q, 8:frame, :])

    first, middle, final = STAGES
    assert first == 2
    tmp[...] = jnp.zeros_like(tmp)

    def inner(p):
        return [functools.partial(few, p, s, j) for s in range(last) for j in range(side)]

    def weave(p, before, extra):
        for at, run in enumerate(inner(p)):
            if at % last == 0:
                few(before, last, at // last)
            run()
            for more in extra.get(at, ()):
                more()

    def some(body, *qs):
        def run():
            for q in qs:
                body(q)

        return run

    order = [(0, 0), (0, 1), (1, 0), (0, 2), (1, 1), (0, 3), (1, 2), (1, 3)]
    order += [(i, j) for i in range(2, side) for j in range(side)]
    order = [(i, j) for i, j in order if i < side and j < side]
    left = {p: list(order) for p in STAGES}

    def hand_on(p):
        if left[p]:
            i, j = left[p].pop(0)
            if i + j == 0:
                pl.semaphore_wait(ready.at[p], len(peers))
            each(4, lambda q: spread(p, i, j, q))

    for run in inner(first):
        run()
    end = last * side - 1
    weave(middle, first, {end - 2: [lambda: each(4, lambda q: swap(q).start())]})
    weave(
        final,
        middle,
        {
            0: [functools.partial(let_in, first)] + [copy.wait for copy in loads] + [some(tall_step, 0)],
            2: [some(tall_step, 1)],
            3: [some(tall_step, 2)],
            5: [some(tall_step, 3)],
            7: [some(join, 0, 1)],
            8: [some(join, 2, 3)],
            end - 1: [functools.partial(let_in, middle), some(functools.partial(wide_step, middle), 0, 1)],
            end: [some(functools.partial(wide_step, middle), 2, 3)],
        },
    )
    few(final, last, 0)
    hand_on(first)
    hand_on(middle)
    few(final, last, 1)
    hand_on(first)
    hand_on(first)
    few(final, last, 2)
    hand_on(middle)
    hand_on(first)
    for j in range(3, side):
        few(final, last, j)
    hand_on(middle)
    let_in(final)
    for q in range(4):
        wide_step(final, q)
        hand_on(STAGES[q % 2])
    while any(left.values()):
        for p in (final, first, middle):
            hand_on(p)
    for p in range(3):
        for q in range(4):
            wait_pieces(ring_send.at[p, q], chips - 1)
            wait_pieces(core_send.at[p, q], chips)
            wait_pieces(all_recv.at[p, q], chips)


def drain_kernel(count, *refs):
    sem = refs[-1]
    copies = []
    for i in range(count):
        here, there = refs[i], refs[count + i]
        parts = PARTS if here.shape[1] % (8 * PARTS) == 0 else 1
        size = here.shape[1] // parts
        for a in range(here.shape[0] if parts > 1 else 1):
            for b in range(parts):
                at = (a, pl.ds(b * size, size)) if parts > 1 else (slice(None),)
                copies.append(pltpu.make_async_copy(here.at[at], there.at[at], sem.at[len(copies)]))
    for copy in copies:
        copy.start()
    for copy in copies:
        copy.wait()


def drain(arrays):
    count = len(arrays)
    return list(
        pl.pallas_call(
            functools.partial(drain_kernel, count),
            out_shape=[jax.ShapeDtypeStruct(a.shape, a.dtype) for a in arrays],
            in_specs=[pl.BlockSpec(memory_space=pltpu.VMEM)] * count,
            out_specs=[pl.BlockSpec(memory_space=pl.ANY)] * count,
            scratch_shapes=[pltpu.SemaphoreType.DMA((2 * PARTS * count,))],
            compiler_params=pltpu.CompilerParams(vmem_limit_bytes=1 << 20),
        )(*arrays)
    )


def solution(mesh):
    n = mesh.shape["dp"]

    def step(*arrays):
        g, w, m, v = (list(arrays[i : i + 3]) for i in (0, 3, 6, 9))
        m[2], v[2] = m[2].swapaxes(0, 1), v[2].swapaxes(0, 1)
        rows, wide = m[0].shape[1:]
        low, _, narrow = m[2].shape
        side = math.isqrt(n // 2)
        half, quarter = rows // 2, narrow // 4
        frame = 2 * low - low // 8 * 8
        assert half * wide == 2 * low * quarter and side * side * 2 == n and low % 8
        dma, regular = pltpu.SemaphoreType.DMA, pltpu.SemaphoreType.REGULAR
        outs = pl.pallas_call(
            functools.partial(step_kernel, n),
            out_shape=[pltpu.VMEM(a.shape, a.dtype) for a in (*w, *m, *v)],
            in_specs=[pl.BlockSpec(memory_space=pltpu.HBM)] * 12,
            out_specs=[pl.BlockSpec(memory_space=pltpu.VMEM)] * 9,
            scratch_shapes=[
                pltpu.VMEM((SLOTS, half, wide), BF16),
                pltpu.VMEM((SLOTS, half, wide), BF16),
                pltpu.VMEM((SLOTS, 2 * low, quarter), BF16),
                pltpu.VMEM((2, rows, wide), BF16),
                pltpu.VMEM((2, rows, wide), BF16),
                pltpu.VMEM((2, frame, narrow), BF16),
                pltpu.VMEM((4, frame, quarter), BF16),
                pltpu.VMEM((4, frame, quarter), F32),
                pltpu.VMEM((4, frame, quarter), F32),
                pltpu.VMEM((4, frame, quarter), F32),
                pltpu.VMEM((frame, quarter), F32),
                dma((3, 4)),
                dma((3, 4, side * side)),
                dma((3, 4)),
                dma((3, 4 * side * side)),
                dma((3, 4)),
                dma((3, SLOTS)),
                dma((9,)),
                dma((4, 4)),
                regular((3,)),
            ],
            compiler_params=pltpu.CompilerParams(
                collective_id=0, has_side_effects=True, vmem_limit_bytes=14 << 20
            ),
        )(*g, *w, *m, *v)
        outs = [*drain(outs[0:1]), *drain(outs[1:2]), *drain(outs[2:3]), *drain(outs[3:])]
        for i in (5, 8):
            outs[i] = outs[i].swapaxes(0, 1)
        return tuple(outs)

    all_of, cut = P(None, None, None), P(None, "dp", None)
    return jax.shard_map(
        step,
        mesh=mesh,
        in_specs=(P(("rep", "dp"), None, None, None),) * 3 + (all_of,) * 3 + (cut,) * 6,
        out_specs=(P("rep", None, None),) * 3 + (P("rep", "dp", None),) * 6,
        check_vma=False,
    )
```

```python
import functools
import math

import jax
import jax.numpy as jnp
from jax import lax
from jax.experimental import pallas as pl
from jax.experimental.pallas import tpu as pltpu
from jax.sharding import PartitionSpec as P

MESH = pl.DeviceIdType.MESH
F32, BF16 = jnp.float32, jnp.bfloat16
SLOTS = 16
PARTS = 8
WIDE, TALL = 0, 1


def adamw(w, m, v, g):
    m = 0.9 * m + 0.1 * g
    v = 0.95 * v + 0.05 * g * g
    step = m * lax.rsqrt(v + 1e-8) + 0.1 * w
    return w - 0.02 * step, m, v


def step_kernel(n, *refs):
    g, w, m, v = (refs[i : i + 3] for i in (0, 3, 6, 9))
    weights, (om, om_tall, ov, ov_tall) = refs[12:14], refs[14:18]
    own, wsl, wsl_tall = refs[18:20], refs[20], refs[21]
    xg, xw, yw, zw, tmp = refs[22:27]
    ring_send, ring_recv, core_send, core_recv, all_recv, own_sem, in_sem, x_sems, ready = refs[27:]

    side = math.isqrt(n // 2)
    last = side - 1
    chips = side * side
    rows = m[0].shape[1]
    low = m[2].shape[0]
    tall = 2 * low
    off = low // 8 * 8
    frame = tall - off
    shift = low - off
    quarter = weights[TALL].shape[2] // 4
    total = 4 * chips
    ahead = 4 * side
    piece_rows = (rows, rows // 2)

    me = lax.axis_index("dp")
    k = lax.rem(me, 2)
    chip = lax.div(me, 2)
    x, y = lax.div(chip, side), lax.rem(chip, side)
    partner = me + 1 - 2 * k

    def wrap(z):
        return lax.rem(z + 2 * side, side)

    class Colour:
        def __init__(self, q):
            self.q = q
            self.a, self.b = lax.div(q, 2), lax.rem(q, 2)
            self.dir = 1 - 2 * self.b
            self.p1, self.p2 = x + self.a * (y - x), y + self.a * (x - y)

        def chip(self, u, v):
            u, v = wrap(u), wrap(v)
            return (u + self.a * (v - u)) * side + v + self.a * (u - v)

        def next1(self):
            return self.chip(self.p1 + self.dir, self.p2) * 2 + k

        def next2(self):
            return self.chip(self.p1, self.p2 + self.dir) * 2 + k

        def back(self, i, j):
            return self.chip(self.p1 - self.dir * i, self.p2 - self.dir * j)

    def within(p, at, core, col):
        if p == WIDE:
            return (pl.ds(pl.multiple_of((at * 2 + core) * rows, rows), rows),)
        return (
            pl.ds(pl.multiple_of(at * tall, 8), tall),
            pl.ds(pl.multiple_of(core * (2 * quarter) + col.b * quarter, quarter), quarter),
        )

    def place(p, at, core, col):
        return (col.q if p == WIDE else col.a, *within(p, at, core, col))

    def from_terms(p, at, core, col, use):
        part = within(p, at, core, col)
        if p == TALL:
            use(g[2].at[(0, col.a, *part)])
            return
        for a in range(2):

            @pl.when(col.a == a)
            def _():
                use(g[a].at[(0, col.b, *part)])

    def remote(src, dst, send, recv, device):
        return pltpu.make_async_remote_copy(
            src_ref=src, dst_ref=dst, send_sem=send, recv_sem=recv, device_id={"dp": device}, device_id_type=MESH
        )

    def wait_pieces(p, sem, count):
        part = weights[WIDE].at[0, pl.ds(0, count * piece_rows[p])]
        pltpu.make_async_copy(part, part, sem).wait()

    def split(t):
        s, j, col = lax.div(t, 4 * side), lax.rem(lax.div(t, 4), side), Colour(lax.rem(t, 4))
        return col, col.back(1 + s, 1 + j)

    def to_partner(p, t):
        col, at = split(t)
        there = weights[p].at[place(p, at, 1 - k, col)]
        send, recv = core_send.at[p, col.q], core_recv.at[p, t]
        from_terms(p, at, 1 - k, col, lambda term: remote(term, there, send, recv, partner).start())

    def load_own(p, t):
        col, at = split(t)
        slot = lax.rem(t, SLOTS)
        here, sem = own[p].at[slot], own_sem.at[p, slot]
        from_terms(p, at, k, col, lambda term: pltpu.make_async_copy(term, here, sem).start())

    def each(count, body):
        lax.fori_loop(0, count, lambda i, c: (body(i), c)[1], 0)

    peers = [
        (wrap(x + dx) * side + wrap(y + dy)) * 2 + k for dx, dy in ((1, 0), (-1, 0), (0, 1), (0, -1))
    ] + [partner]
    barrier = pltpu.get_barrier_semaphore()
    for peer in peers:
        pl.semaphore_signal(barrier, inc=1, device_id={"dp": peer}, device_id_type=MESH)
    each(SLOTS, functools.partial(load_own, TALL))
    pl.semaphore_wait(barrier, len(peers))
    each(ahead, functools.partial(to_partner, TALL))
    each(SLOTS, functools.partial(load_own, WIDE))

    here = pl.ds(pl.multiple_of(me * rows, rows), rows)
    rim = pl.ds(pl.multiple_of(chip * tall + off * k, 8), frame)
    pairs = [(w[2].at[:, rim], wsl_tall), (m[2], om_tall), (v[2], ov_tall)]
    for a in range(2):
        half = pl.ds(2 * a, 2)
        pairs += [(w[a].at[:, here], wsl.at[half]), (m[a], om.at[half]), (v[a], ov.at[half])]
    loads = [pltpu.make_async_copy(src, dst, in_sem.at[i]) for i, (src, dst) in enumerate(pairs)]
    for copy in loads:
        copy.start()

    def reduce(p, s, j, q):
        col = Colour(q)
        at = col.back(1 + s, 1 + j)
        t = (s * side + j) * 4 + q
        slot = lax.rem(t, SLOTS)
        i = place(p, at, k, col)
        out = weights[p]
        wait_pieces(p, core_recv.at[p, t], 1)
        wait_pieces(p, own_sem.at[p, slot], 1)
        so_far = out[i].astype(F32) + own[p][slot].astype(F32)
        came = [(s - 1) * side + j] if s > 0 else []
        if s == last and j > 0:
            came.append(last * side + j - 1)
        for r in came:
            wait_pieces(p, ring_recv.at[p, q, r], 1)
            so_far += out[place(p, r, 1 - k, col)].astype(F32)
        out[i] = so_far.astype(BF16)
        if s < last or j < last:
            r = s * side + j
            there = out.at[place(p, r, 1 - k, col)]
            device = col.next2() if s == last else col.next1()
            remote(out.at[i], there, ring_send.at[p, q], ring_recv.at[p, q, r], device).start()
        if (s * side + j) * 4 + SLOTS < total:
            load_own(p, t + SLOTS)
        if (s * side + j) * 4 + ahead < total:
            to_partner(p, t + ahead)
        if p == TALL and s == last - 1:
            to_partner(WIDE, t + 2 * ahead - total)

    def few(p, s, j):
        each(4, lambda q: reduce(p, s, j, q))

    def let_in(p):
        for q in range(4):
            wait_pieces(p, ring_send.at[p, q], chips - 1)
            wait_pieces(p, core_send.at[p, q], chips)
        for peer in peers:
            pl.semaphore_signal(ready.at[p], inc=1, device_id={"dp": peer}, device_id_type=MESH)

    def spread(p, i, j, q):
        col = Colour(q)
        at = col.back(i, j)
        if i + j > 0:
            wait_pieces(p, ring_recv.at[p, q, i * side + j], 1)
        part = weights[p].at[place(p, at, k, col)]
        if i == 0 and j < last:
            remote(part, part, ring_send.at[p, q], ring_recv.at[p, q, j + 1], col.next2()).start()
        if i < last:
            remote(part, part, ring_send.at[p, q], ring_recv.at[p, q, (i + 1) * side + j], col.next1()).start()
        remote(part, part, core_send.at[p, q], all_recv.at[p, q], partner).start()

    def wide_step(q):
        i = place(WIDE, chip, k, Colour(q))
        new, new_m, new_v = adamw(wsl[q].astype(F32), om[q], ov[q], weights[WIDE][i].astype(F32))
        weights[WIDE][i] = new.astype(BF16)
        om[q] = new_m
        ov[q] = new_v

    def swap(q):
        col = Colour(q)
        part = weights[TALL].at[
            col.a,
            pl.ds(pl.multiple_of(chip * tall + off * (1 - k), 8), frame),
            pl.ds(pl.multiple_of(k * (2 * quarter) + col.b * quarter, quarter), quarter),
        ]
        return remote(part, xg.at[q], x_sems.at[0, q], x_sems.at[1, q], partner)

    def give(q):
        return remote(zw.at[q], xw.at[q], x_sems.at[2, q], x_sems.at[3, q], partner)

    def tall_step(q):
        a, b = q // 2, q % 2
        swap(q).wait()
        for core in range(2):

            @pl.when(k == core)
            def _():
                for mine in (True, False):
                    side_of = core if mine else 1 - core
                    cols = pl.ds(side_of * 2 * quarter + b * quarter, quarter)
                    if mine:
                        grad = weights[TALL][a, pl.ds(pl.multiple_of(chip * tall + off * core, 8), frame), cols]
                    else:
                        grad = xg[q]
                    at = slice(shift * core, shift * core + low)
                    new, new_m, new_v = adamw(
                        wsl_tall[a, :, cols].astype(F32)[at],
                        om_tall[:, a, cols],
                        ov_tall[:, a, cols],
                        grad.astype(F32)[at],
                    )
                    om_tall[:, a, cols] = new_m
                    ov_tall[:, a, cols] = new_v
                    tmp[at, :] = new
                    (yw if mine else zw)[q] = tmp[...]

        give(q).start()

    def join(q):
        col = Colour(q)
        give(q).wait()
        cols = pl.ds(pl.multiple_of(k * 2 * quarter + col.b * quarter, quarter), quarter)
        base = chip * tall

        def put(start, value):
            part = pl.ds(pl.multiple_of(base + start, 8), value.shape[0])
            weights[TALL][col.a, part, cols] = value.astype(BF16)

        for core in range(2):

            @pl.when(k == core)
            def _():
                top, bottom = (yw, xw) if core == 0 else (xw, yw)
                put(0, top[q, 0:off, :])
                row = lax.broadcasted_iota(jnp.int32, (8, quarter), 0)
                put(off, jnp.where(row < shift, top[q, off : off + 8, :], bottom[q, 0:8, :]))
                put(off + 8, bottom[q, 8:frame, :])

    order = [(0, 0), (0, 1), (1, 0), (0, 2), (1, 1), (0, 3), (1, 2), (1, 3)]
    order += [(i, j) for i in range(2, side) for j in range(side)]
    order = [(i, j) for i, j in order if i < side and j < side]
    left = [list(order), list(order)]

    def hand_on(p, count=1):
        for i, j in left[p][:count]:
            if i + j == 0:
                pl.semaphore_wait(ready.at[p], len(peers))
            each(4, lambda q, i=i, j=j: spread(p, i, j, q))
        del left[p][:count]

    tmp[...] = jnp.zeros_like(tmp)
    steps = [(s, j) for s in range(last) for j in range(side)]
    for s, j in steps:
        few(TALL, s, j)
    for at, (s, j) in enumerate(steps):
        if at % 2 == 0 and at // 2 < side:
            few(TALL, last, at // 2)
        few(WIDE, s, j)
        if at == 2 * last:
            each(4, lambda q: swap(q).start())
        if at == 2 * last + 1:
            let_in(TALL)
            for copy in loads:
                copy.wait()
            tall_step(0)
        if at == 2 * last + 2:
            tall_step(1)
        if at == 2 * last + 3:
            tall_step(2)
            tall_step(3)
        if at == 2 * last + 4:
            join(0)
            join(1)
        if at == 2 * last + 5:
            join(2)
            join(3)
    for j in range(side):
        few(WIDE, last, j)
        hand_on(TALL, 2 if j < last else 1)
    let_in(WIDE)
    for q in range(4):
        wide_step(q)
        hand_on(TALL)
    while left[WIDE] or left[TALL]:
        hand_on(WIDE)
        hand_on(TALL)
    for p in (TALL, WIDE):
        for q in range(4):
            wait_pieces(p, ring_send.at[p, q], chips - 1)
            wait_pieces(p, core_send.at[p, q], chips)
            wait_pieces(p, all_recv.at[p, q], chips)


def drain_kernel(count, *refs):
    sem = refs[-1]
    copies = []

    def copy(src, dst):
        copies.append(pltpu.make_async_copy(src, dst, sem.at[len(copies)]))

    at = count
    for here in refs[:count]:
        layers = 0
        while layers < here.shape[0]:
            there = refs[at]
            at += 1
            if there.shape == here.shape and there.shape[0] > 2:
                copy(here, there)
            else:
                size = there.shape[1] // PARTS
                size = size if size % 8 == 0 else there.shape[1]
                for a in range(there.shape[0]):
                    for b in range(0, there.shape[1], size):
                        copy(here.at[layers + a, pl.ds(b, size)], there.at[a, pl.ds(b, size)])
            layers += there.shape[0]
    for one in copies:
        one.start()
    for one in copies:
        one.wait()


def drain(arrays, like):
    return pl.pallas_call(
        functools.partial(drain_kernel, len(arrays)),
        out_shape=[jax.ShapeDtypeStruct(a.shape, a.dtype) for a in like],
        in_specs=[pl.BlockSpec(memory_space=pltpu.VMEM)] * len(arrays),
        out_specs=[pl.BlockSpec(memory_space=pl.ANY)] * len(like),
        scratch_shapes=[pltpu.SemaphoreType.DMA((2 * PARTS * len(like),))],
        compiler_params=pltpu.CompilerParams(vmem_limit_bytes=1 << 20),
    )(*arrays)


def solution(mesh):
    n = mesh.shape["dp"]

    def step(*arrays):
        g, w, m, v = (list(arrays[i : i + 3]) for i in (0, 3, 6, 9))
        m[2], v[2] = m[2].swapaxes(0, 1), v[2].swapaxes(0, 1)
        layers, rows, wide = m[0].shape
        low, _, narrow = m[2].shape
        side = math.isqrt(n // 2)
        quarter = narrow // 4
        frame = 2 * low - low // 8 * 8
        assert rows * wide == 4 * low * quarter and side * side * 2 == n and low % 8 and layers == 2
        dma, regular = pltpu.SemaphoreType.DMA, pltpu.SemaphoreType.REGULAR
        both = (2 * layers, *w[0].shape[1:])
        blocks = (2 * layers, rows, wide)
        outs = pl.pallas_call(
            functools.partial(step_kernel, n),
            out_shape=[
                pltpu.VMEM(both, BF16),
                pltpu.VMEM(w[2].shape, BF16),
                pltpu.VMEM(blocks, F32),
                pltpu.VMEM(m[2].shape, F32),
                pltpu.VMEM(blocks, F32),
                pltpu.VMEM(v[2].shape, F32),
            ],
            in_specs=[pl.BlockSpec(memory_space=pltpu.HBM)] * 12,
            out_specs=[pl.BlockSpec(memory_space=pltpu.VMEM)] * 6,
            scratch_shapes=[
                pltpu.VMEM((SLOTS, rows, wide), BF16),
                pltpu.VMEM((SLOTS, 2 * low, quarter), BF16),
                pltpu.VMEM(blocks, BF16),
                pltpu.VMEM((layers, frame, narrow), BF16),
                pltpu.VMEM((4, frame, quarter), BF16),
                pltpu.VMEM((4, frame, quarter), F32),
                pltpu.VMEM((4, frame, quarter), F32),
                pltpu.VMEM((4, frame, quarter), F32),
                pltpu.VMEM((frame, quarter), F32),
                dma((2, 4)),
                dma((2, 4, side * side)),
                dma((2, 4)),
                dma((2, 4 * side * side)),
                dma((2, 4)),
                dma((2, SLOTS)),
                dma((9,)),
                dma((4, 4)),
                regular((2,)),
            ],
            compiler_params=pltpu.CompilerParams(
                collective_id=0, has_side_effects=True, vmem_limit_bytes=14 << 20
            ),
        )(*g, *w, *m, *v)
        gate, up = drain(outs[:1], w[:2])
        down, *moments = drain(outs[1:], [w[2], *m, *v])
        for i in (2, 5):
            moments[i] = moments[i].swapaxes(0, 1)
        return gate, up, down, *moments

    all_of, cut = P(None, None, None), P(None, "dp", None)
    return jax.shard_map(
        step,
        mesh=mesh,
        in_specs=(P(("rep", "dp"), None, None, None),) * 3 + (all_of,) * 3 + (cut,) * 6,
        out_specs=(P("rep", None, None),) * 3 + (P("rep", "dp", None),) * 6,
        check_vma=False,
    )
```

```python
import functools
import math

import jax
import jax.numpy as jnp
from jax import lax
from jax.experimental import pallas as pl
from jax.experimental.pallas import tpu as pltpu
from jax.sharding import PartitionSpec as P

MESH = pl.DeviceIdType.MESH
F32, BF16 = jnp.float32, jnp.bfloat16
SLOTS = 16
PARTS = 1
WIDE, TALL = 0, 1


def adamw(w, m, v, g):
    m = 0.9 * m + 0.1 * g
    v = 0.95 * v + 0.05 * g * g
    step = m * lax.rsqrt(v + 1e-8) + 0.1 * w
    return w - 0.02 * step, m, v


def step_kernel(n, *refs):
    g, w, m, v = (refs[i : i + 3] for i in (0, 3, 6, 9))
    weights, (om, om_tall, ov, ov_tall) = refs[12:14], refs[14:18]
    own, wsl, wsl_tall = refs[18:20], refs[20], refs[21]
    xg, xw, yw, zw, tmp = refs[22:27]
    ring_send, ring_recv, core_send, core_recv, all_recv, own_sem, in_sem, x_sems, ready = refs[27:]

    side = math.isqrt(n // 2)
    last = side - 1
    chips = side * side
    rows = m[0].shape[1]
    low = m[2].shape[0]
    tall = 2 * low
    off = low // 8 * 8
    frame = tall - off
    shift = low - off
    quarter = weights[TALL].shape[2] // 4
    total = 4 * chips
    ahead = 4 * side
    piece_rows = (rows, rows // 2)

    me = lax.axis_index("dp")
    k = lax.rem(me, 2)
    chip = lax.div(me, 2)
    x, y = lax.div(chip, side), lax.rem(chip, side)
    partner = me + 1 - 2 * k

    def wrap(z):
        return lax.rem(z + 2 * side, side)

    class Colour:
        def __init__(self, q):
            self.q = q
            self.a, self.b = lax.div(q, 2), lax.rem(q, 2)
            self.dir = 1 - 2 * self.b
            self.p1, self.p2 = x + self.a * (y - x), y + self.a * (x - y)

        def chip(self, u, v):
            u, v = wrap(u), wrap(v)
            return (u + self.a * (v - u)) * side + v + self.a * (u - v)

        def next1(self):
            return self.chip(self.p1 + self.dir, self.p2) * 2 + k

        def next2(self):
            return self.chip(self.p1, self.p2 + self.dir) * 2 + k

        def back(self, i, j):
            return self.chip(self.p1 - self.dir * i, self.p2 - self.dir * j)

    def within(p, at, core, col):
        if p == WIDE:
            return (pl.ds(pl.multiple_of((at * 2 + core) * rows, rows), rows),)
        return (
            pl.ds(pl.multiple_of(at * tall, 8), tall),
            pl.ds(pl.multiple_of(core * (2 * quarter) + col.b * quarter, quarter), quarter),
        )

    def place(p, at, core, col):
        return (col.q if p == WIDE else col.a, *within(p, at, core, col))

    def from_terms(p, at, core, col, use):
        part = within(p, at, core, col)
        if p == TALL:
            use(g[2].at[(0, col.a, *part)])
            return
        for a in range(2):

            @pl.when(col.a == a)
            def _():
                use(g[a].at[(0, col.b, *part)])

    def remote(src, dst, send, recv, device):
        return pltpu.make_async_remote_copy(
            src_ref=src, dst_ref=dst, send_sem=send, recv_sem=recv, device_id={"dp": device}, device_id_type=MESH
        )

    def wait_pieces(p, sem, count):
        part = weights[WIDE].at[0, pl.ds(0, count * piece_rows[p])]
        pltpu.make_async_copy(part, part, sem).wait()

    def split(t):
        s, j, col = lax.div(t, 4 * side), lax.rem(lax.div(t, 4), side), Colour(lax.rem(t, 4))
        return col, col.back(1 + s, 1 + j)

    def to_partner(p, t):
        col, at = split(t)
        there = weights[p].at[place(p, at, 1 - k, col)]
        send, recv = core_send.at[p, col.q], core_recv.at[p, t]
        from_terms(p, at, 1 - k, col, lambda term: remote(term, there, send, recv, partner).start())

    def load_own(p, t):
        col, at = split(t)
        slot = lax.rem(t, SLOTS)
        here, sem = own[p].at[slot], own_sem.at[p, slot]
        from_terms(p, at, k, col, lambda term: pltpu.make_async_copy(term, here, sem).start())

    def each(count, body):
        lax.fori_loop(0, count, lambda i, c: (body(i), c)[1], 0)

    peers = [
        (wrap(x + dx) * side + wrap(y + dy)) * 2 + k for dx, dy in ((1, 0), (-1, 0), (0, 1), (0, -1))
    ] + [partner]
    barrier = pltpu.get_barrier_semaphore()
    for peer in peers:
        pl.semaphore_signal(barrier, inc=1, device_id={"dp": peer}, device_id_type=MESH)
    each(SLOTS, functools.partial(load_own, TALL))
    pl.semaphore_wait(barrier, len(peers))
    each(ahead, functools.partial(to_partner, TALL))

    here = pl.ds(pl.multiple_of(me * rows, rows), rows)
    rim = pl.ds(pl.multiple_of(chip * tall + off * k, 8), frame)
    pairs = [(w[2].at[:, rim], wsl_tall), (m[2], om_tall), (v[2], ov_tall)]
    for a in range(2):
        half = pl.ds(2 * a, 2)
        pairs += [(w[a].at[:, here], wsl.at[half]), (m[a], om.at[half]), (v[a], ov.at[half])]
    loads = [pltpu.make_async_copy(src, dst, in_sem.at[i]) for i, (src, dst) in enumerate(pairs)]
    def reduce(p, s, j, q):
        col = Colour(q)
        at = col.back(1 + s, 1 + j)
        t = (s * side + j) * 4 + q
        slot = lax.rem(t, SLOTS)
        i = place(p, at, k, col)
        out = weights[p]
        wait_pieces(p, core_recv.at[p, t], 1)
        wait_pieces(p, own_sem.at[p, slot], 1)
        so_far = out[i].astype(F32) + own[p][slot].astype(F32)
        came = [(s - 1) * side + j] if s > 0 else []
        if s == last and j > 0:
            came.append(last * side + j - 1)
        for r in came:
            wait_pieces(p, ring_recv.at[p, q, r], 1)
            so_far += out[place(p, r, 1 - k, col)].astype(F32)
        out[i] = so_far.astype(BF16)
        if s < last or j < last:
            r = s * side + j
            there = out.at[place(p, r, 1 - k, col)]
            device = col.next2() if s == last else col.next1()
            remote(out.at[i], there, ring_send.at[p, q], ring_recv.at[p, q, r], device).start()
        if (s * side + j) * 4 + SLOTS < total:
            load_own(p, t + SLOTS)
        if (s * side + j) * 4 + ahead < total:
            to_partner(p, t + ahead)
        if p == TALL and s == last - 1:
            to_partner(WIDE, t + 2 * ahead - total)

    def few(p, s, j):
        each(4, lambda q: reduce(p, s, j, q))

    def let_in(p):
        for q in range(4):
            wait_pieces(p, ring_send.at[p, q], chips - 1)
            wait_pieces(p, core_send.at[p, q], chips)
        for peer in peers:
            pl.semaphore_signal(ready.at[p], inc=1, device_id={"dp": peer}, device_id_type=MESH)

    def spread(p, i, j, q):
        col = Colour(q)
        at = col.back(i, j)
        if i + j > 0:
            wait_pieces(p, ring_recv.at[p, q, i * side + j], 1)
        part = weights[p].at[place(p, at, k, col)]
        if i == 0 and j < last:
            remote(part, part, ring_send.at[p, q], ring_recv.at[p, q, j + 1], col.next2()).start()
        if i < last:
            remote(part, part, ring_send.at[p, q], ring_recv.at[p, q, (i + 1) * side + j], col.next1()).start()
        remote(part, part, core_send.at[p, q], all_recv.at[p, q], partner).start()

    def wide_step(q):
        i = place(WIDE, chip, k, Colour(q))
        new, new_m, new_v = adamw(wsl[q].astype(F32), om[q], ov[q], weights[WIDE][i].astype(F32))
        weights[WIDE][i] = new.astype(BF16)
        om[q] = new_m
        ov[q] = new_v

    def swap(q):
        col = Colour(q)
        part = weights[TALL].at[
            col.a,
            pl.ds(pl.multiple_of(chip * tall + off * (1 - k), 8), frame),
            pl.ds(pl.multiple_of(k * (2 * quarter) + col.b * quarter, quarter), quarter),
        ]
        return remote(part, xg.at[q], x_sems.at[0, q], x_sems.at[1, q], partner)

    def give(q):
        return remote(zw.at[q], xw.at[q], x_sems.at[2, q], x_sems.at[3, q], partner)

    def tall_step(q):
        a, b = q // 2, q % 2
        swap(q).wait()
        for core in range(2):

            @pl.when(k == core)
            def _():
                for mine in (True, False):
                    side_of = core if mine else 1 - core
                    cols = pl.ds(side_of * 2 * quarter + b * quarter, quarter)
                    if mine:
                        grad = weights[TALL][a, pl.ds(pl.multiple_of(chip * tall + off * core, 8), frame), cols]
                    else:
                        grad = xg[q]
                    at = slice(shift * core, shift * core + low)
                    new, new_m, new_v = adamw(
                        wsl_tall[a, :, cols].astype(F32)[at],
                        om_tall[:, a, cols],
                        ov_tall[:, a, cols],
                        grad.astype(F32)[at],
                    )
                    om_tall[:, a, cols] = new_m
                    ov_tall[:, a, cols] = new_v
                    tmp[at, :] = new
                    (yw if mine else zw)[q] = tmp[...]

        give(q).start()

    def join(q):
        col = Colour(q)
        give(q).wait()
        cols = pl.ds(pl.multiple_of(k * 2 * quarter + col.b * quarter, quarter), quarter)
        base = chip * tall

        def put(start, value):
            part = pl.ds(pl.multiple_of(base + start, 8), value.shape[0])
            weights[TALL][col.a, part, cols] = value.astype(BF16)

        for core in range(2):

            @pl.when(k == core)
            def _():
                top, bottom = (yw, xw) if core == 0 else (xw, yw)
                put(0, top[q, 0:off, :])
                row = lax.broadcasted_iota(jnp.int32, (8, quarter), 0)
                put(off, jnp.where(row < shift, top[q, off : off + 8, :], bottom[q, 0:8, :]))
                put(off + 8, bottom[q, 8:frame, :])

    order = [(0, 0), (0, 1), (1, 0), (0, 2), (1, 1), (0, 3), (1, 2), (1, 3)]
    order += [(i, j) for i in range(2, side) for j in range(side)]
    order = [(i, j) for i, j in order if i < side and j < side]
    left = [list(order), list(order)]

    def hand_on(p, count=1):
        for i, j in left[p][:count]:
            if i + j == 0:
                pl.semaphore_wait(ready.at[p], len(peers))
            each(4, lambda q, i=i, j=j: spread(p, i, j, q))
        del left[p][:count]

    tmp[...] = jnp.zeros_like(tmp)
    steps = [(s, j) for s in range(last) for j in range(side)]
    for s, j in steps:
        few(TALL, s, j)
        if (s, j) == (1, 0):
            each(SLOTS, functools.partial(load_own, WIDE))
            for copy in loads:
                copy.start()
    for at, (s, j) in enumerate(steps):
        if at % 2 == 0 and at // 2 < side:
            few(TALL, last, at // 2)
        few(WIDE, s, j)
        if at == 2 * last:
            each(4, lambda q: swap(q).start())
        if at == 2 * last + 1:
            let_in(TALL)
            for copy in loads:
                copy.wait()
            tall_step(0)
        if at == 2 * last + 2:
            tall_step(1)
        if at == 2 * last + 3:
            tall_step(2)
            tall_step(3)
        if at == 2 * last + 4:
            join(0)
            join(1)
        if at == 2 * last + 5:
            join(2)
            join(3)
    for j in range(side):
        hand_on(TALL, 2 if j > 0 else 1)
        few(WIDE, last, j)
        if j == 0:
            hand_on(TALL, 1)
    let_in(WIDE)
    for q in range(4):
        wide_step(q)
        hand_on(TALL)
    while left[WIDE] or left[TALL]:
        hand_on(WIDE)
        hand_on(TALL)
    for p in (TALL, WIDE):
        for q in range(4):
            wait_pieces(p, ring_send.at[p, q], chips - 1)
            wait_pieces(p, core_send.at[p, q], chips)
            wait_pieces(p, all_recv.at[p, q], chips)


def drain_kernel(count, *refs):
    sem = refs[-1]
    copies = []

    def copy(src, dst):
        copies.append(pltpu.make_async_copy(src, dst, sem.at[len(copies)]))

    at = count
    for here in refs[:count]:
        layers = 0
        while layers < here.shape[0]:
            there = refs[at]
            at += 1
            if there.shape == here.shape and there.shape[0] > 2:
                copy(here, there)
            else:
                size = there.shape[1] // PARTS
                size = size if size % 8 == 0 else there.shape[1]
                for a in range(there.shape[0]):
                    for b in range(0, there.shape[1], size):
                        copy(here.at[layers + a, pl.ds(b, size)], there.at[a, pl.ds(b, size)])
            layers += there.shape[0]
    for one in copies:
        one.start()
    for one in copies:
        one.wait()


def drain(arrays, like):
    return pl.pallas_call(
        functools.partial(drain_kernel, len(arrays)),
        out_shape=[jax.ShapeDtypeStruct(a.shape, a.dtype) for a in like],
        in_specs=[pl.BlockSpec(memory_space=pltpu.VMEM)] * len(arrays),
        out_specs=[pl.BlockSpec(memory_space=pl.ANY)] * len(like),
        scratch_shapes=[pltpu.SemaphoreType.DMA((2 * PARTS * len(like),))],
        compiler_params=pltpu.CompilerParams(vmem_limit_bytes=1 << 20),
    )(*arrays)


def solution(mesh):
    n = mesh.shape["dp"]

    def step(*arrays):
        g, w, m, v = (list(arrays[i : i + 3]) for i in (0, 3, 6, 9))
        m[2], v[2] = m[2].swapaxes(0, 1), v[2].swapaxes(0, 1)
        layers, rows, wide = m[0].shape
        low, _, narrow = m[2].shape
        side = math.isqrt(n // 2)
        quarter = narrow // 4
        frame = 2 * low - low // 8 * 8
        assert rows * wide == 4 * low * quarter and side * side * 2 == n and low % 8 and layers == 2
        dma, regular = pltpu.SemaphoreType.DMA, pltpu.SemaphoreType.REGULAR
        both = (2 * layers, *w[0].shape[1:])
        blocks = (2 * layers, rows, wide)
        outs = pl.pallas_call(
            functools.partial(step_kernel, n),
            out_shape=[
                pltpu.VMEM(both, BF16),
                pltpu.VMEM(w[2].shape, BF16),
                pltpu.VMEM(blocks, F32),
                pltpu.VMEM(m[2].shape, F32),
                pltpu.VMEM(blocks, F32),
                pltpu.VMEM(v[2].shape, F32),
            ],
            in_specs=[pl.BlockSpec(memory_space=pltpu.HBM)] * 12,
            out_specs=[pl.BlockSpec(memory_space=pltpu.VMEM)] * 6,
            scratch_shapes=[
                pltpu.VMEM((SLOTS, rows, wide), BF16),
                pltpu.VMEM((SLOTS, 2 * low, quarter), BF16),
                pltpu.VMEM(blocks, BF16),
                pltpu.VMEM((layers, frame, narrow), BF16),
                pltpu.VMEM((4, frame, quarter), BF16),
                pltpu.VMEM((4, frame, quarter), F32),
                pltpu.VMEM((4, frame, quarter), F32),
                pltpu.VMEM((4, frame, quarter), F32),
                pltpu.VMEM((frame, quarter), F32),
                dma((2, 4)),
                dma((2, 4, side * side)),
                dma((2, 4)),
                dma((2, 4 * side * side)),
                dma((2, 4)),
                dma((2, SLOTS)),
                dma((9,)),
                dma((4, 4)),
                regular((2,)),
            ],
            compiler_params=pltpu.CompilerParams(
                collective_id=0, has_side_effects=True, vmem_limit_bytes=14 << 20
            ),
        )(*g, *w, *m, *v)
        gate, up = drain(outs[:1], w[:2])
        down, *moments = drain(outs[1:], [w[2], *m, *v])
        for i in (2, 5):
            moments[i] = moments[i].swapaxes(0, 1)
        return gate, up, down, *moments

    all_of, cut = P(None, None, None), P(None, "dp", None)
    return jax.shard_map(
        step,
        mesh=mesh,
        in_specs=(P(("rep", "dp"), None, None, None),) * 3 + (all_of,) * 3 + (cut,) * 6,
        out_specs=(P("rep", None, None),) * 3 + (P("rep", "dp", None),) * 6,
        check_vma=False,
    )
```

```python
import functools
import math

import jax
import jax.numpy as jnp
from jax import lax
from jax.experimental import pallas as pl
from jax.experimental.pallas import tpu as pltpu
from jax.sharding import PartitionSpec as P

MESH = pl.DeviceIdType.MESH
F32, BF16 = jnp.float32, jnp.bfloat16
SLOTS = 16
PARTS = 1
WIDE, TALL = 0, 1


def adamw(w, m, v, g):
    m = 0.9 * m + 0.1 * g
    v = 0.95 * v + 0.05 * g * g
    step = m * lax.rsqrt(v + 1e-8) + 0.1 * w
    return w - 0.02 * step, m, v


def step_kernel(n, *refs):
    g, w, m, v = (refs[i : i + 3] for i in (0, 3, 6, 9))
    weights, (om, om_tall, ov, ov_tall) = refs[12:14], refs[14:18]
    own, wsl, wsl_tall = refs[18:20], refs[20], refs[21]
    xg, xw, yw, zw, tmp = refs[22:27]
    ring_send, ring_recv, core_send, core_recv, all_recv, own_sem, in_sem, x_sems, ready = refs[27:]

    side = math.isqrt(n // 2)
    last = side - 1
    chips = side * side
    rows = m[0].shape[1]
    low = m[2].shape[0]
    tall = 2 * low
    off = low // 8 * 8
    frame = tall - off
    shift = low - off
    quarter = weights[TALL].shape[2] // 4
    total = 4 * chips
    ahead = 4 * side
    piece_rows = (rows, rows // 2)

    me = lax.axis_index("dp")
    k = lax.rem(me, 2)
    chip = lax.div(me, 2)
    x, y = lax.div(chip, side), lax.rem(chip, side)
    partner = me + 1 - 2 * k

    def wrap(z):
        return lax.rem(z + 2 * side, side)

    class Colour:
        def __init__(self, q):
            self.q = q
            self.a, self.b = lax.div(q, 2), lax.rem(q, 2)
            self.dir = 1 - 2 * self.b
            self.p1, self.p2 = x + self.a * (y - x), y + self.a * (x - y)

        def chip(self, u, v):
            u, v = wrap(u), wrap(v)
            return (u + self.a * (v - u)) * side + v + self.a * (u - v)

        def next1(self):
            return self.chip(self.p1 + self.dir, self.p2) * 2 + k

        def next2(self):
            return self.chip(self.p1, self.p2 + self.dir) * 2 + k

        def back(self, i, j):
            return self.chip(self.p1 - self.dir * i, self.p2 - self.dir * j)

    def within(p, at, core, col):
        if p == WIDE:
            return (pl.ds(pl.multiple_of((at * 2 + core) * rows, rows), rows),)
        return (
            pl.ds(pl.multiple_of(at * tall, 8), tall),
            pl.ds(pl.multiple_of(core * (2 * quarter) + col.b * quarter, quarter), quarter),
        )

    def place(p, at, core, col):
        return (col.q if p == WIDE else col.a, *within(p, at, core, col))

    def from_terms(p, at, core, col, use):
        part = within(p, at, core, col)
        if p == TALL:
            use(g[2].at[(0, col.a, *part)])
            return
        for a in range(2):

            @pl.when(col.a == a)
            def _():
                use(g[a].at[(0, col.b, *part)])

    def remote(src, dst, send, recv, device):
        return pltpu.make_async_remote_copy(
            src_ref=src, dst_ref=dst, send_sem=send, recv_sem=recv, device_id={"dp": device}, device_id_type=MESH
        )

    def wait_pieces(p, sem, count):
        part = weights[WIDE].at[0, pl.ds(0, count * piece_rows[p])]
        pltpu.make_async_copy(part, part, sem).wait()

    def split(t):
        s, j, col = lax.div(t, 4 * side), lax.rem(lax.div(t, 4), side), Colour(lax.rem(t, 4))
        return col, col.back(1 + s, 1 + j)

    def to_partner(p, t):
        col, at = split(t)
        there = weights[p].at[place(p, at, 1 - k, col)]
        send, recv = core_send.at[p, col.q], core_recv.at[p, t]
        from_terms(p, at, 1 - k, col, lambda term: remote(term, there, send, recv, partner).start())

    def load_own(p, t):
        col, at = split(t)
        slot = lax.rem(t, SLOTS)
        here, sem = own[p].at[slot], own_sem.at[p, slot]
        from_terms(p, at, k, col, lambda term: pltpu.make_async_copy(term, here, sem).start())

    def each(count, body):
        lax.fori_loop(0, count, lambda i, c: (body(i), c)[1], 0)

    peers = [
        (wrap(x + dx) * side + wrap(y + dy)) * 2 + k for dx, dy in ((1, 0), (-1, 0), (0, 1), (0, -1))
    ] + [partner]
    barrier = pltpu.get_barrier_semaphore()
    for peer in peers:
        pl.semaphore_signal(barrier, inc=1, device_id={"dp": peer}, device_id_type=MESH)
    each(SLOTS, functools.partial(load_own, TALL))
    pl.semaphore_wait(barrier, len(peers))
    each(ahead, functools.partial(to_partner, TALL))

    here = pl.ds(pl.multiple_of(me * rows, rows), rows)
    rim = pl.ds(pl.multiple_of(chip * tall + off * k, 8), frame)
    pairs = [(w[2].at[:, rim], wsl_tall), (m[2], om_tall), (v[2], ov_tall)]
    for a in range(2):
        half = pl.ds(2 * a, 2)
        pairs += [(w[a].at[:, here], wsl.at[half]), (m[a], om.at[half]), (v[a], ov.at[half])]
    loads = [pltpu.make_async_copy(src, dst, in_sem.at[i]) for i, (src, dst) in enumerate(pairs)]
    def reduce(p, s, j, q):
        col = Colour(q)
        at = col.back(1 + s, 1 + j)
        t = (s * side + j) * 4 + q
        slot = lax.rem(t, SLOTS)
        i = place(p, at, k, col)
        out = weights[p]
        wait_pieces(p, core_recv.at[p, t], 1)
        wait_pieces(p, own_sem.at[p, slot], 1)
        so_far = out[i].astype(F32) + own[p][slot].astype(F32)
        came = [(s - 1) * side + j] if s > 0 else []
        if s == last and j > 0:
            came.append(last * side + j - 1)
        for r in came:
            wait_pieces(p, ring_recv.at[p, q, r], 1)
            so_far += out[place(p, r, 1 - k, col)].astype(F32)
        out[i] = so_far.astype(BF16)
        if s < last or j < last:
            r = s * side + j
            there = out.at[place(p, r, 1 - k, col)]
            device = col.next2() if s == last else col.next1()
            remote(out.at[i], there, ring_send.at[p, q], ring_recv.at[p, q, r], device).start()
        if (s * side + j) * 4 + SLOTS < total:
            load_own(p, t + SLOTS)
        if (s * side + j) * 4 + ahead < total:
            to_partner(p, t + ahead)
        if p == TALL and s == last - 1:
            to_partner(WIDE, t + 2 * ahead - total)

    def few(p, s, j):
        each(4, lambda q: reduce(p, s, j, q))

    def let_in(p):
        for q in range(4):
            wait_pieces(p, ring_send.at[p, q], chips - 1)
            wait_pieces(p, core_send.at[p, q], chips)
        for peer in peers:
            pl.semaphore_signal(ready.at[p], inc=1, device_id={"dp": peer}, device_id_type=MESH)

    def spread(p, i, j, q):
        col = Colour(q)
        at = col.back(i, j)
        if i + j > 0:
            wait_pieces(p, ring_recv.at[p, q, i * side + j], 1)
        part = weights[p].at[place(p, at, k, col)]
        if i == 0 and j < last:
            remote(part, part, ring_send.at[p, q], ring_recv.at[p, q, j + 1], col.next2()).start()
        if i < last:
            remote(part, part, ring_send.at[p, q], ring_recv.at[p, q, (i + 1) * side + j], col.next1()).start()
        remote(part, part, core_send.at[p, q], all_recv.at[p, q], partner).start()

    def wide_step(q):
        i = place(WIDE, chip, k, Colour(q))
        new, new_m, new_v = adamw(wsl[q].astype(F32), om[q], ov[q], weights[WIDE][i].astype(F32))
        weights[WIDE][i] = new.astype(BF16)
        om[q] = new_m
        ov[q] = new_v

    def swap(q):
        col = Colour(q)
        part = weights[TALL].at[
            col.a,
            pl.ds(pl.multiple_of(chip * tall + off * (1 - k), 8), frame),
            pl.ds(pl.multiple_of(k * (2 * quarter) + col.b * quarter, quarter), quarter),
        ]
        return remote(part, xg.at[q], x_sems.at[0, q], x_sems.at[1, q], partner)

    def give(q):
        return remote(zw.at[q], xw.at[q], x_sems.at[2, q], x_sems.at[3, q], partner)

    def tall_step(q):
        a, b = q // 2, q % 2
        swap(q).wait()
        for core in range(2):

            @pl.when(k == core)
            def _():
                for mine in (True, False):
                    side_of = core if mine else 1 - core
                    cols = pl.ds(side_of * 2 * quarter + b * quarter, quarter)
                    if mine:
                        grad = weights[TALL][a, pl.ds(pl.multiple_of(chip * tall + off * core, 8), frame), cols]
                    else:
                        grad = xg[q]
                    at = slice(shift * core, shift * core + low)
                    new, new_m, new_v = adamw(
                        wsl_tall[a, :, cols].astype(F32)[at],
                        om_tall[:, a, cols],
                        ov_tall[:, a, cols],
                        grad.astype(F32)[at],
                    )
                    om_tall[:, a, cols] = new_m
                    ov_tall[:, a, cols] = new_v
                    tmp[at, :] = new
                    (yw if mine else zw)[q] = tmp[...]

        give(q).start()

    def join(q):
        col = Colour(q)
        give(q).wait()
        cols = pl.ds(pl.multiple_of(k * 2 * quarter + col.b * quarter, quarter), quarter)
        base = chip * tall

        def put(start, value):
            part = pl.ds(pl.multiple_of(base + start, 8), value.shape[0])
            weights[TALL][col.a, part, cols] = value.astype(BF16)

        for core in range(2):

            @pl.when(k == core)
            def _():
                top, bottom = (yw, xw) if core == 0 else (xw, yw)
                put(0, top[q, 0:off, :])
                row = lax.broadcasted_iota(jnp.int32, (8, quarter), 0)
                put(off, jnp.where(row < shift, top[q, off : off + 8, :], bottom[q, 0:8, :]))
                put(off + 8, bottom[q, 8:frame, :])

    order = [(0, 0), (0, 1), (1, 0), (0, 2), (1, 1), (0, 3), (1, 2), (1, 3)]
    order += [(i, j) for i in range(2, side) for j in range(side)]
    order = [(i, j) for i, j in order if i < side and j < side]
    left = [list(order), list(order)]

    def hand_on(p, count=1):
        for i, j in left[p][:count]:
            if i + j == 0:
                pl.semaphore_wait(ready.at[p], len(peers))
            each(4, lambda q, i=i, j=j: spread(p, i, j, q))
        del left[p][:count]

    tmp[...] = jnp.zeros_like(tmp)
    steps = [(s, j) for s in range(last) for j in range(side)]
    for s, j in steps:
        few(TALL, s, j)
        if (s, j) == (1, 0):
            each(SLOTS, functools.partial(load_own, WIDE))
            for copy in loads:
                copy.start()
    for at, (s, j) in enumerate(steps):
        if at % 2 == 0 and at // 2 < side:
            few(TALL, last, at // 2)
        few(WIDE, s, j)
        if at == 2 * last:
            each(4, lambda q: swap(q).start())
        if at == 2 * last + 1:
            let_in(TALL)
            for copy in loads:
                copy.wait()
            tall_step(0)
        if at == 2 * last + 2:
            tall_step(1)
        if at == 2 * last + 3:
            tall_step(2)
            tall_step(3)
        if at == 2 * last + 4:
            join(0)
            join(1)
        if at == 2 * last + 5:
            join(2)
            join(3)
    for j in range(side):
        hand_on(TALL, 2 if j > 0 else 1)
        few(WIDE, last, j)
        if j == 0:
            hand_on(TALL, 1)
    let_in(WIDE)
    for q in range(4):
        wide_step(q)
        hand_on(TALL)
    while left[WIDE]:
        hand_on(WIDE)
        if len(left[TALL]) > side:
            hand_on(TALL)
    hand_on(TALL, len(left[TALL]))
    for p in (TALL, WIDE):
        for q in range(4):
            wait_pieces(p, ring_send.at[p, q], chips - 1)
            wait_pieces(p, core_send.at[p, q], chips)
            wait_pieces(p, all_recv.at[p, q], chips)


def drain_kernel(count, *refs):
    sem = refs[-1]
    copies = []

    def copy(src, dst):
        copies.append(pltpu.make_async_copy(src, dst, sem.at[len(copies)]))

    at = count
    for here in refs[:count]:
        layers = 0
        while layers < here.shape[0]:
            there = refs[at]
            at += 1
            if there.shape == here.shape and there.shape[0] > 2:
                copy(here, there)
            else:
                size = there.shape[1] // PARTS
                size = size if size % 8 == 0 else there.shape[1]
                for a in range(there.shape[0]):
                    for b in range(0, there.shape[1], size):
                        copy(here.at[layers + a, pl.ds(b, size)], there.at[a, pl.ds(b, size)])
            layers += there.shape[0]
    for one in copies:
        one.start()
    for one in copies:
        one.wait()


def drain(arrays, like):
    return pl.pallas_call(
        functools.partial(drain_kernel, len(arrays)),
        out_shape=[jax.ShapeDtypeStruct(a.shape, a.dtype) for a in like],
        in_specs=[pl.BlockSpec(memory_space=pltpu.VMEM)] * len(arrays),
        out_specs=[pl.BlockSpec(memory_space=pl.ANY)] * len(like),
        scratch_shapes=[pltpu.SemaphoreType.DMA((2 * PARTS * len(like),))],
        compiler_params=pltpu.CompilerParams(vmem_limit_bytes=1 << 20),
    )(*arrays)


def solution(mesh):
    n = mesh.shape["dp"]

    def step(*arrays):
        g, w, m, v = (list(arrays[i : i + 3]) for i in (0, 3, 6, 9))
        m[2], v[2] = m[2].swapaxes(0, 1), v[2].swapaxes(0, 1)
        layers, rows, wide = m[0].shape
        low, _, narrow = m[2].shape
        side = math.isqrt(n // 2)
        quarter = narrow // 4
        frame = 2 * low - low // 8 * 8
        assert rows * wide == 4 * low * quarter and side * side * 2 == n and low % 8 and layers == 2
        dma, regular = pltpu.SemaphoreType.DMA, pltpu.SemaphoreType.REGULAR
        both = (2 * layers, *w[0].shape[1:])
        blocks = (2 * layers, rows, wide)
        outs = pl.pallas_call(
            functools.partial(step_kernel, n),
            out_shape=[
                pltpu.VMEM(both, BF16),
                pltpu.VMEM(w[2].shape, BF16),
                pltpu.VMEM(blocks, F32),
                pltpu.VMEM(m[2].shape, F32),
                pltpu.VMEM(blocks, F32),
                pltpu.VMEM(v[2].shape, F32),
            ],
            in_specs=[pl.BlockSpec(memory_space=pltpu.HBM)] * 12,
            out_specs=[pl.BlockSpec(memory_space=pltpu.VMEM)] * 6,
            scratch_shapes=[
                pltpu.VMEM((SLOTS, rows, wide), BF16),
                pltpu.VMEM((SLOTS, 2 * low, quarter), BF16),
                pltpu.VMEM(blocks, BF16),
                pltpu.VMEM((layers, frame, narrow), BF16),
                pltpu.VMEM((4, frame, quarter), BF16),
                pltpu.VMEM((4, frame, quarter), F32),
                pltpu.VMEM((4, frame, quarter), F32),
                pltpu.VMEM((4, frame, quarter), F32),
                pltpu.VMEM((frame, quarter), F32),
                dma((2, 4)),
                dma((2, 4, side * side)),
                dma((2, 4)),
                dma((2, 4 * side * side)),
                dma((2, 4)),
                dma((2, SLOTS)),
                dma((9,)),
                dma((4, 4)),
                regular((2,)),
            ],
            compiler_params=pltpu.CompilerParams(
                collective_id=0, has_side_effects=True, vmem_limit_bytes=14 << 20
            ),
        )(*g, *w, *m, *v)
        gate, up = drain(outs[:1], w[:2])
        down, *moments = drain(outs[1:], [w[2], *m, *v])
        for i in (2, 5):
            moments[i] = moments[i].swapaxes(0, 1)
        return gate, up, down, *moments

    all_of, cut = P(None, None, None), P(None, "dp", None)
    return jax.shard_map(
        step,
        mesh=mesh,
        in_specs=(P(("rep", "dp"), None, None, None),) * 3 + (all_of,) * 3 + (cut,) * 6,
        out_specs=(P("rep", None, None),) * 3 + (P("rep", "dp", None),) * 6,
        check_vma=False,
    )
```
